512 devices in a mesh: pb: 8 (over x, core), ka: 64 (over z, y).
Axes of the slice: x: 4, y: 8, z: 8, core: 2. Of those that a mesh axis runs over, the one named last changes fastest.
Arguments:
- coupling: bfloat16 [8, 64, 128, 32, 384], P('pb', 'ka'), may hold values from -0.796875 to 0.796875
- phonon_occ: float32 [8, 64, 128, 12], P('pb', 'ka'), may hold values from 0.1 to 1
- band_window: int32 [8, 64, 128, 32], P('pb', 'ka'), may hold values 0 or 1
- pair_count: int32 [8, 64, 64], P('pb', 'ka'), may hold values from 0 to 2, as said below
- k_target: int32 [8, 64, 128], P('pb', 'ka'), may hold values from 0 to 127
- kq_source: int32 [8, 64, 128], P('pb', 'ka'), may hold values from 0 to 127
- velocity: float32 [3, 32, 8192], P(None, None, 'ka'), may hold values from -6 to 6
- lifetime: float32 [32, 8192], P(None, 'ka'), may hold values from 0.5 to 2
Outputs:
- deviation: float32 [3, 32, 8192], P(None, None, 'ka')
The draws below stay inside these ranges and needn't reach their ends.
Inputs may be any that keep to these rules, and one draw needn't show every extreme that they name: pair_count[p, a, d] is the number of live tile slots among slots d * 2 to d * 2 + 1 of device (p, a); in every q-group p some owner d receives 2 live tiles from every source.
All inputs are finite; a program needn't handle non-finite values. No bound on the sum of `band_window` on one device may be relied on, other than what follows from the above.
Results may differ from the reference program's by a relative error of at most 0.012.
Values may be sent and summed in bfloat16 or wider, within the bound.
No kernel may reach another device: no remote copies, remote signals or barrier semaphores. Data moves between devices by JAX's collectives and lax.ppermute only.
A program may use at most 64 MiB of HBM per device.

```python
import math
import jax
import jax.numpy as jnp
from jax import lax

BANDS = 32
MODES = 12
K_DEV = 128
TILE_SLOTS = 2
ITERS = 4
KPOINTS = 8192
TILES = 128
N_PB = 8
N_KA = 64


def draw_pair_count(key, part):
    first_key, second_key = jax.random.split(jax.random.fold_in(key, 17), 2)
    base = jax.random.randint(first_key, (N_PB, N_KA, N_KA), 0, TILE_SLOTS + 1)
    busiest = jax.random.randint(second_key, (N_PB, 1, 1), 0, N_KA)
    column = jnp.arange(N_KA)[None, None, :] == busiest
    return jnp.where(column, TILE_SLOTS, base).astype(jnp.int32)


def set_ends(drawn, rng, least, high):
    index_at = [jax.random.randint(jax.random.fold_in(rng, axis), (), 0, length) for axis, length in enumerate(drawn.shape)]
    main_axis = drawn.shape.index(max(drawn.shape))
    neighbour = index_at[:main_axis] + [(index_at[main_axis] + 1) % drawn.shape[main_axis]] + index_at[main_axis + 1:]
    return drawn.at[tuple(index_at)].set(least).at[tuple(neighbour)].set(high)


def levels(own_key, shape, cuts, low, top_value):
    level, own = 1.0, jax.random.fold_in(own_key, 6)
    for position, blocks in cuts:
        heights = jnp.exp(jax.random.uniform(jax.random.fold_in(own, position), (blocks,), jnp.float32, low / len(cuts), top_value / len(cuts)))
        level = level * jnp.repeat(heights, shape[position] // blocks).reshape([-1 if axis == position else 1 for axis in range(len(shape))])
    return level


def gaussian(own_key, shape, spread, bound, pieces=(), held_as=jnp.bfloat16):
    array = spread * jax.random.normal(own_key, shape, jnp.float32)
    if pieces:
        array = array * levels(own_key, shape, pieces, -0.22, 0.18)
    return jnp.clip(array, -bound, bound).astype(held_as)


def setup_inputs(seed: int = 0) -> dict:
    seeds = jax.random.split(jax.random.key(seed), 9)
    return {
        "coupling": gaussian(seeds[0], (N_PB, N_KA, TILES, BANDS, BANDS * MODES), 0.1, 0.796875, ((0, 8), (1, 64))),
        "phonon_occ": jnp.clip(jnp.exp(math.log(1.0) - 2.3025851 * jax.random.uniform(seeds[1], (N_PB, N_KA, TILES, MODES), jnp.float32) ** levels(seeds[1], (N_PB, N_KA, TILES, MODES), ((0, 8), (1, 64)), -0.2, 0.2)), 0.1, 1.0),
        "band_window": set_ends((jax.random.randint(seeds[2], (N_PB, N_KA, TILES, BANDS), 0, 4) < 3).astype(jnp.int32), jax.random.fold_in(seeds[2], 1), 0, 1),
        "pair_count": draw_pair_count(jax.random.fold_in(seeds[8], 71), 0),
        "k_target": set_ends(jax.random.randint(seeds[4], (N_PB, N_KA, TILES), 0, K_DEV), jax.random.fold_in(seeds[4], 1), 0, K_DEV - 1).astype(jnp.int32),
        "kq_source": set_ends(jax.random.randint(seeds[5], (N_PB, N_KA, TILES), 0, K_DEV), jax.random.fold_in(seeds[5], 1), 0, K_DEV - 1).astype(jnp.int32),
        "velocity": gaussian(seeds[6], (3, BANDS, KPOINTS), 1.0, 6.0, ((2, 64),), jnp.float32),
        "lifetime": jnp.clip(jnp.exp(math.log(2.0) - 1.3862944 * jax.random.uniform(seeds[7], (BANDS, KPOINTS), jnp.float32) ** levels(seeds[7], (BANDS, KPOINTS), ((1, 64),), -0.2, 0.2)), 0.5, 2.0),
    }


def weigh_tile(coupling_tile, occ_tile, slot_live, window):
    squared = coupling_tile.astype(jnp.float32) * coupling_tile.astype(jnp.float32)
    squared = squared.reshape(squared.shape[0], BANDS, BANDS, MODES)
    summed = jnp.sum(squared * occ_tile[:, None, None, :], axis=3)
    masked = slot_live[:, None] * window
    return (summed * masked[:, :, None]).astype(jnp.bfloat16)


def reference(coupling, phonon_occ, band_window, pair_count, k_target, kq_source, velocity, lifetime):
    tile_count = N_KA * TILE_SLOTS
    block_count = N_PB * N_KA
    slot_live = (jnp.arange(TILE_SLOTS)[None, None, None, :] < pair_count[:, :, :, None])
    slot_live = slot_live.reshape(block_count, tile_count).astype(jnp.float32)
    coupling_blocks = coupling.reshape(block_count, tile_count, BANDS, BANDS * MODES)
    occ_blocks = phonon_occ.reshape(block_count, tile_count, MODES)
    window_blocks = band_window.reshape(block_count, tile_count, BANDS).astype(jnp.float32)
    target_blocks = k_target.reshape(block_count, tile_count)
    source_blocks = kq_source.reshape(block_count, tile_count)
    block_owner = (jnp.arange(block_count) % N_KA).astype(jnp.int32)
    owner = (jnp.arange(tile_count) // TILE_SLOTS).astype(jnp.int32)
    deviation = lifetime[None] * velocity
    for iteration in range(ITERS):
        rounded = deviation.astype(jnp.bfloat16)

        def block_term(scatter_total, items):
            coupling_tile, occ_tile, live_tile, window, target, source_local, source_block = items
            weight = weigh_tile(coupling_tile, occ_tile, live_tile, window)
            columns = (source_block * K_DEV + source_local).astype(jnp.int32)
            chosen = jnp.take(rounded, columns, axis=2)
            contribution = jnp.einsum("tnm,dmt->dnt", weight.astype(jnp.float32), chosen.astype(jnp.float32), precision=lax.Precision.HIGHEST)
            global_k = (owner * K_DEV + target).astype(jnp.int32)
            return scatter_total.at[:, :, global_k].add(contribution), None

        start_total = jnp.zeros((3, BANDS, K_DEV * N_KA), jnp.float32)
        scattering, unused = lax.scan(block_term, start_total, (coupling_blocks, occ_blocks, slot_live, window_blocks, target_blocks, source_blocks, block_owner))
        deviation = lifetime[None] * (velocity + scattering)
    return deviation
```

```python
import jax
import jax.numpy as jnp
from jax import lax
from jax.experimental import pallas as pl
from jax.experimental.pallas import tpu as pltpu
from jax.sharding import PartitionSpec as P

MODES = 12
TILE_SLOTS = 2
ITERS = 4
BANDS = 32
ROWS = 3 * BANDS
TILES = 128
LANES = BANDS * MODES
CHUNKS = 8
F32 = jnp.float32
BF16 = jnp.bfloat16


def iota(shape, axis):
    return lax.broadcasted_iota(jnp.int32, shape, axis)


def updated(velocity, lifetime, scattering):
    parts = []
    for i in range(3):
        rows = slice(i * BANDS, (i + 1) * BANDS)
        total = velocity[rows, :]
        if scattering is not None:
            total = total + scattering[rows, :]
        parts.append(lifetime * total)
    return jnp.concatenate(parts, axis=0)


def send_terms(deviation, weight_ref, source_ref, target_ref, chosen_ref, term_ref, out_ref):
    picks = (iota((TILES, TILES), 0) == source_ref[...]).astype(F32).astype(BF16)
    chosen_ref[...] = jnp.dot(deviation.astype(BF16), picks, preferred_element_type=F32)
    for i in range(3):
        total = None
        for m in range(BANDS):
            term = weight_ref[pl.ds(m * BANDS, BANDS), :] * chosen_ref[pl.ds(i * BANDS + m, 1), :]
            total = term if total is None else total + term
        term_ref[pl.ds(i * BANDS, BANDS), :] = total
    tail = jnp.where(iota((BANDS, TILES), 0) == 0, target_ref[...].astype(F32), 0.0)
    term_ref[pl.ds(ROWS, BANDS), :] = tail
    out_ref[...] = term_ref[...].T.astype(BF16)


def weight_kernel(
    coupling_hbm, occ_ref, window_ref, count_ref, source_ref, target_ref, velocity_ref, lifetime_ref,
    weight_ref, out_ref,
    tiles, flat, occ_wide, occ_pad, chosen_ref, term_ref, sems,
):
    step = TILES // CHUNKS
    copies = []
    for c in range(CHUNKS):
        part = pl.ds(c * step, step)
        copies.append(pltpu.make_async_copy(coupling_hbm.at[part], tiles.at[part], sems.at[c]))
        copies[-1].start()
    occ_pad[...] = jnp.zeros_like(occ_pad)
    occ_pad[pl.ds(0, MODES), :] = occ_ref[...]
    spread = (iota((16, LANES), 1) % MODES == iota((16, LANES), 0)).astype(F32)
    occ_wide[...] = lax.dot_general(
        occ_pad[...].T, spread, (((1,), (0,)), ((), ())),
        precision=lax.Precision.HIGHEST, preferred_element_type=F32,
    )
    gather = (iota((LANES, TILES), 0) // MODES == iota((LANES, TILES), 1) % BANDS).astype(F32).astype(BF16)
    group = iota((1, 1, TILES), 2) // BANDS
    for c in range(CHUNKS):
        copies[c].wait()
        part = tiles[pl.ds(c * step, step)]
        occ = occ_wide[pl.ds(c * step, step), :].astype(BF16)
        scaled = part * part * occ[:, None, :]
        summed = jnp.dot(
            scaled.reshape(step * BANDS, LANES), gather, preferred_element_type=F32
        ).reshape(step, 4, 8, TILES)
        merged = summed[:, 0]
        for j in range(1, 4):
            merged = jnp.where(group == j, summed[:, j], merged)
        flat[pl.ds(c * step * 8, step * 8), :] = merged.reshape(step * 8, TILES)
    count = count_ref[...].astype(F32).astype(BF16)
    owner = (iota((64, TILES), 1) // TILE_SLOTS == iota((64, TILES), 0)).astype(F32).astype(BF16)
    live = jnp.dot(jnp.broadcast_to(count, (8, 64)), owner, preferred_element_type=F32)
    slot = (iota((8, TILES), 1) % TILE_SLOTS).astype(F32)
    live = (slot < live).astype(F32)
    mask = window_ref[...].astype(F32) * live[0:1, :]
    for q in range(8):
        turned = flat[pl.ds(q, TILES, stride=8), :].T
        for j in range(4):
            n = j * 8 + q
            weight_ref[pl.ds(n, BANDS, stride=BANDS), :] = (
                turned[j * BANDS : (j + 1) * BANDS, :] * mask[n : n + 1, :]
            )
    deviation = updated(velocity_ref[...], lifetime_ref[...], None)
    send_terms(deviation, weight_ref, source_ref, target_ref, chosen_ref, term_ref, out_ref)


def step_kernel(
    parts_ref, weight_ref, source_ref, target_ref, velocity_ref, lifetime_ref, out_ref, chosen_ref, term_ref
):
    deviation = updated(velocity_ref[...], lifetime_ref[...], sum_parts(parts_ref))
    send_terms(deviation, weight_ref, source_ref, target_ref, chosen_ref, term_ref, out_ref)


def sum_parts(parts_ref):
    total = parts_ref[0].astype(F32)
    for p in range(1, parts_ref.shape[0]):
        total = total + parts_ref[p].astype(F32)
    return total


def final_kernel(parts_ref, velocity_ref, lifetime_ref, out_ref):
    out_ref[...] = updated(velocity_ref[...], lifetime_ref[...], sum_parts(parts_ref))


def receive_kernel(terms_ref, out_ref):
    terms = terms_ref[...].astype(F32)
    target = terms[:, ROWS : ROWS + 1].astype(jnp.int32)
    onehot = (iota((TILES, TILES), 1) == target).astype(F32).astype(BF16)
    turned = terms.T[:ROWS, :].astype(BF16)
    partial_sum = jnp.dot(turned, onehot, preferred_element_type=F32).astype(BF16)
    for p in range(out_ref.shape[0]):
        out_ref[p] = partial_sum


VMEM = pl.BlockSpec(memory_space=pltpu.VMEM)


def call(body, name, ins, outs, scratch=(), limit=4 << 20, flops=1000000):
    return pl.pallas_call(
        body,
        name=name,
        in_specs=ins,
        out_specs=[VMEM] * len(outs),
        out_shape=[jax.ShapeDtypeStruct(s, d) for s, d in outs],
        scratch_shapes=list(scratch),
        compiler_params=pltpu.CompilerParams(vmem_limit_bytes=limit),
        cost_estimate=pl.CostEstimate(flops=flops, bytes_accessed=1 << 20, transcendentals=0),
    )


def shards(coupling, phonon_occ, band_window, pair_count, k_target, kq_source, velocity, lifetime):
    groups = lax.axis_size("pb")
    small = [pltpu.VMEM((ROWS, TILES), F32), pltpu.VMEM((TILES, TILES), F32)]
    velocity = velocity.reshape(ROWS, TILES)
    source = kq_source.reshape(1, TILES)
    target = k_target.reshape(1, TILES)
    weight, terms = call(
        weight_kernel, "weights", [pl.BlockSpec(memory_space=pl.ANY)] + [VMEM] * 7,
        [((BANDS * BANDS, TILES), F32), ((TILES, TILES), BF16)],
        [
            pltpu.VMEM((TILES, BANDS, LANES), BF16),
            pltpu.VMEM((TILES * 8, TILES), F32),
            pltpu.VMEM((TILES, LANES), F32),
            pltpu.VMEM((16, TILES), F32),
            *small,
            pltpu.SemaphoreType.DMA((CHUNKS,)),
        ],
        limit=16 << 20,
    )(
        coupling[0, 0], phonon_occ[0, 0].T, band_window[0, 0].T, pair_count[0], source, target, velocity, lifetime,
    )
    for iteration in range(ITERS):
        if iteration:
            (terms,) = call(step_kernel, "step", [VMEM] * 6, [((TILES, TILES), BF16)], small)(
                parts, weight, source, target, velocity, lifetime
            )
        arrived = lax.all_to_all(
            terms.reshape(-1, TILE_SLOTS, TILES), "ka", split_axis=0, concat_axis=0, tiled=True
        ).reshape(TILES, TILES)
        (copies,) = call(receive_kernel, "receive", [VMEM], [((groups, ROWS, TILES), BF16)])(arrived)
        parts = lax.all_to_all(copies, "pb", split_axis=0, concat_axis=0, tiled=True)
    (deviation,) = call(final_kernel, "final", [VMEM] * 3, [((ROWS, TILES), F32)])(
        parts, velocity, lifetime
    )
    return deviation.reshape(3, BANDS, TILES)


def solution(mesh):
    placed = (
        P("pb", "ka", None, None, None),
        P("pb", "ka", None, None),
        P("pb", "ka", None, None),
        P("pb", "ka", None),
        P("pb", "ka", None),
        P("pb", "ka", None),
        P(None, None, "ka"),
        P(None, "ka"),
    )
    return jax.shard_map(
        shards, mesh=mesh, in_specs=placed, out_specs=P(None, None, "ka"), check_vma=False
    )
```

```python
import jax
import jax.numpy as jnp
from jax import lax
from jax.experimental import pallas as pl
from jax.experimental.pallas import tpu as pltpu
from jax.sharding import PartitionSpec as P

MODES = 12
TILE_SLOTS = 2
ITERS = 4
BANDS = 32
ROWS = 3 * BANDS
TILES = 128
LANES = BANDS * MODES
CHUNKS = 8
F32 = jnp.float32
BF16 = jnp.bfloat16


def iota(shape, axis):
    return lax.broadcasted_iota(jnp.int32, shape, axis)


def updated(state_ref, scattering):
    lifetime = state_ref[pl.ds(ROWS, BANDS), :]
    parts = []
    for i in range(3):
        rows = slice(i * BANDS, (i + 1) * BANDS)
        total = state_ref[rows, :]
        if scattering is not None:
            total = total + scattering[rows, :]
        parts.append(lifetime * total)
    return jnp.concatenate(parts, axis=0)


def send_terms(deviation, weight_ref, index_ref, chosen_ref, half_ref, term_ref, out_ref):
    picks = (iota((TILES, TILES), 0) == index_ref[0:1, :]).astype(F32).astype(BF16)
    chosen_ref[...] = jnp.dot(deviation.astype(BF16), picks, preferred_element_type=F32)
    first = iota((8, TILES), 0) < 4
    for i in range(3):
        pairs = []
        for m in range(0, BANDS, 2):
            row = i * BANDS + m
            low = jnp.broadcast_to(chosen_ref[pl.ds(row, 1), :], (8, TILES))
            high = jnp.broadcast_to(chosen_ref[pl.ds(row + 1, 1), :], (8, TILES))
            pairs.append(jnp.where(first, low, high))
        for q in range(8):
            total = None
            for m, pair in enumerate(pairs):
                term = weight_ref[pl.ds(q * TILES + m * 8, 8), :] * pair
                total = term if total is None else total + term
            half_ref[pl.ds(i * 64 + q * 8, 8), :] = total
        for j in range(4):
            term_ref[pl.ds(i * BANDS + j * 8, 8), :] = (
                half_ref[pl.ds(i * 64 + j, 8, stride=8), :]
                + half_ref[pl.ds(i * 64 + j + 4, 8, stride=8), :]
            )
    target = index_ref[1:2, :].astype(F32)
    term_ref[pl.ds(ROWS, BANDS), :] = jnp.where(iota((BANDS, TILES), 0) == 0, target, 0.0)
    out_ref[...] = term_ref[...].T.astype(BF16)


def weight_kernel(
    coupling, occ, window, count, source, target, velocity, lifetime,
    weight_ref, out_ref, state_ref, index_ref,
    tiles, flat, occ_wide, occ_pad, window_ref, count_ref, mask_ref, chosen_ref, half_ref, term_ref, sems, small_sems,
):
    small = []
    for place, (origin, into) in enumerate((
        *((occ.at[v], occ_pad.at[pl.ds(v, 1)]) for v in range(MODES)),
        (count, count_ref),
        (window, window_ref),
        (velocity, state_ref.at[pl.ds(0, ROWS)]),
        (lifetime, state_ref.at[pl.ds(ROWS, BANDS)]),
        (source, index_ref.at[pl.ds(0, 1)]),
        (target, index_ref.at[pl.ds(1, 1)]),
    )):
        small.append(pltpu.make_async_copy(origin, into, small_sems.at[place]))
    for copy in small[:MODES]:
        copy.start()
    step = TILES // CHUNKS
    copies = []
    for c in range(CHUNKS):
        part = pl.ds(c * step, step)
        copies.append(pltpu.make_async_copy(coupling.at[part], tiles.at[part], sems.at[c]))
        copies[-1].start()
        if c == 0:
            for copy in small[MODES:]:
                copy.start()
    spread = (iota((16, LANES), 1) % MODES == iota((16, LANES), 0)).astype(F32).astype(BF16)
    gather = (iota((LANES, TILES), 0) // MODES == iota((LANES, TILES), 1) // 4).astype(F32).astype(BF16)
    group = iota((1, TILES), 1) % 4
    for copy in small[:MODES]:
        copy.wait()
    valid = iota((16, TILES), 0) < MODES
    occ_rows = jnp.where(valid, occ_pad[...], 0.0).T.astype(BF16)
    occ_wide[...] = jnp.dot(occ_rows, spread, preferred_element_type=F32)
    summed = None
    for c in range(CHUNKS + 1):
        before = summed
        if c < CHUNKS:
            copies[c].wait()
            rows = []
            for t in range(c * step, (c + 1) * step):
                tile = tiles[t]
                wide = jnp.broadcast_to(occ_wide[pl.ds(t, 1), :], (BANDS, LANES)).astype(BF16)
                rows.append(tile * tile * wide)
            summed = jnp.dot(jnp.concatenate(rows, axis=0), gather, preferred_element_type=F32)
        for t in range(step if c else 0):
            merged = before[t * BANDS : t * BANDS + 8, :]
            for j in range(1, 4):
                row = t * BANDS + j * 8
                merged = jnp.where(group == j, before[row : row + 8, :], merged)
            flat[pl.ds(((c - 1) * step + t) * 8, 8), :] = merged
    for copy in small[MODES:]:
        copy.wait()
    count = count_ref[...].astype(F32).astype(BF16)
    owner = (iota((64, TILES), 1) // TILE_SLOTS == iota((64, TILES), 0)).astype(F32).astype(BF16)
    live = jnp.dot(jnp.broadcast_to(count, (8, 64)), owner, preferred_element_type=F32)
    slot = (iota((8, TILES), 1) % TILE_SLOTS).astype(F32)
    live = (slot < live).astype(F32)
    mask = window_ref[...].astype(F32) * live[0:1, :]
    mask_ref[pl.ds(0, BANDS), :] = mask
    mask_ref[pl.ds(BANDS, BANDS), :] = mask
    for q in range(8):
        turned = flat[pl.ds(q, TILES, stride=8), :].T
        rows = mask_ref[pl.ds(q, 8, stride=8), :]
        for m in range(16):
            weight_ref[pl.ds(q * TILES + m * 8, 8), :] = turned[m * 8 : m * 8 + 8, :] * rows
    deviation = updated(state_ref, None)
    send_terms(deviation, weight_ref, index_ref, chosen_ref, half_ref, term_ref, out_ref)


def step_kernel(parts_ref, weight_ref, state_ref, index_ref, out_ref, chosen_ref, half_ref, term_ref):
    deviation = updated(state_ref, sum_parts(parts_ref))
    send_terms(deviation, weight_ref, index_ref, chosen_ref, half_ref, term_ref, out_ref)


def sum_parts(parts_ref):
    total = parts_ref[0].astype(F32)
    for p in range(1, parts_ref.shape[0]):
        total = total + parts_ref[p].astype(F32)
    return total


def final_kernel(parts_ref, state_ref, out_ref):
    out_ref[...] = updated(state_ref, sum_parts(parts_ref))


def receive_kernel(terms_ref, out_ref):
    terms = terms_ref[...].astype(F32)
    target = terms[:, ROWS : ROWS + 1].astype(jnp.int32)
    onehot = (iota((TILES, TILES), 1) == target).astype(F32).astype(BF16)
    turned = terms.T[:ROWS, :].astype(BF16)
    partial_sum = jnp.dot(turned, onehot, preferred_element_type=F32).astype(BF16)
    for p in range(out_ref.shape[0]):
        out_ref[p] = partial_sum


VMEM = pl.BlockSpec(memory_space=pltpu.VMEM)


def call(body, name, ins, outs, scratch=(), limit=4 << 20, flops=1000000):
    return pl.pallas_call(
        body,
        name=name,
        in_specs=ins,
        out_specs=[VMEM] * len(outs),
        out_shape=[jax.ShapeDtypeStruct(s, d) for s, d in outs],
        scratch_shapes=list(scratch),
        compiler_params=pltpu.CompilerParams(vmem_limit_bytes=limit),
        cost_estimate=pl.CostEstimate(flops=flops, bytes_accessed=1 << 20, transcendentals=0),
    )


def shards(coupling, phonon_occ, band_window, pair_count, k_target, kq_source, velocity, lifetime):
    groups = lax.axis_size("pb")
    small = [
        pltpu.VMEM((ROWS, TILES), F32), pltpu.VMEM((3 * 64, TILES), F32), pltpu.VMEM((TILES, TILES), F32)
    ]
    weight, terms, state, index = call(
        weight_kernel, "weights", [pl.BlockSpec(memory_space=pltpu.HBM)] * 8,
        [
            ((BANDS * BANDS, TILES), F32), ((TILES, TILES), BF16),
            ((TILES, TILES), F32), ((8, TILES), jnp.int32),
        ],
        [
            pltpu.VMEM((TILES, BANDS, LANES), BF16),
            pltpu.VMEM((TILES * 8, TILES), F32),
            pltpu.VMEM((TILES, LANES), F32),
            pltpu.VMEM((16, TILES), F32),
            pltpu.VMEM((BANDS, TILES), jnp.int32),
            pltpu.VMEM((1, 64), jnp.int32),
            pltpu.VMEM((2 * BANDS, TILES), F32),
            *small,
            pltpu.SemaphoreType.DMA((CHUNKS,)),
            pltpu.SemaphoreType.DMA((MODES + 6,)),
        ],
        limit=16 << 20,
    )(*(pltpu.with_memory_space_constraint(x, pltpu.HBM) for x in (
        coupling[0, 0], phonon_occ.transpose(0, 3, 1, 2).reshape(MODES, 1, TILES), band_window[0, 0].T, pair_count[0],
        kq_source.reshape(1, TILES), k_target.reshape(1, TILES), velocity.reshape(ROWS, TILES), lifetime,
    )))
    for iteration in range(ITERS):
        if iteration:
            (terms,) = call(step_kernel, "step", [VMEM] * 4, [((TILES, TILES), BF16)], small)(
                parts, weight, state, index
            )
        arrived = lax.all_to_all(
            terms.reshape(-1, TILE_SLOTS, TILES), "ka", split_axis=0, concat_axis=0, tiled=True
        ).reshape(TILES, TILES)
        (copies,) = call(receive_kernel, "receive", [VMEM], [((groups, ROWS, TILES), BF16)])(arrived)
        parts = lax.all_to_all(copies, "pb", split_axis=0, concat_axis=0, tiled=True)
    (deviation,) = call(final_kernel, "final", [VMEM] * 2, [((ROWS, TILES), F32)])(parts, state)
    return deviation.reshape(3, BANDS, TILES)


def solution(mesh):
    placed = (
        P("pb", "ka", None, None, None),
        P("pb", "ka", None, None),
        P("pb", "ka", None, None),
        P("pb", "ka", None),
        P("pb", "ka", None),
        P("pb", "ka", None),
        P(None, None, "ka"),
        P(None, "ka"),
    )
    return jax.shard_map(
        shards, mesh=mesh, in_specs=placed, out_specs=P(None, None, "ka"), check_vma=False
    )
```

```python
import jax
import jax.numpy as jnp
from jax import lax
from jax.experimental import pallas as pl
from jax.experimental.pallas import tpu as pltpu
from jax.sharding import PartitionSpec as P


MODES = 12
TILE_SLOTS = 2
ITERS = 4
BANDS = 32
ROWS = 3 * BANDS
TILES = 128
LANES = BANDS * MODES
CHUNKS = 8
WIDE = BANDS * BANDS
F32 = jnp.float32
BF16 = jnp.bfloat16


def iota(shape, axis):
    return lax.broadcasted_iota(jnp.int32, shape, axis)


def band_terms(weight, base, pairs, half_ref, term_ref, slot):
    for q in range(8):
        total = None
        for m, pair in enumerate(pairs):
            term = weight[pl.ds(q * TILES + m * 8, 8), :].astype(F32) * pair
            total = term if total is None else total + term
        half_ref[pl.ds(base + q * 8, 8), :] = total
    for j in range(4):
        term_ref[pl.ds(slot * BANDS + j * 8, 8), :] = (
            half_ref[pl.ds(base + j, 8, stride=8), :] + half_ref[pl.ds(base + j + 4, 8, stride=8), :]
        )


def band_pairs(chosen_ref, slot):
    first = iota((8, TILES), 0) < 4
    pairs = []
    for m in range(0, BANDS, 2):
        row = slot * BANDS + m
        low = jnp.broadcast_to(chosen_ref[pl.ds(row, 1), :], (8, TILES))
        high = jnp.broadcast_to(chosen_ref[pl.ds(row + 1, 1), :], (8, TILES))
        pairs.append(jnp.where(first, low, high))
    return pairs


def onehot(equal):
    return equal.astype(F32).astype(BF16)


def weight_kernel(
    coupling, occ, window, count, source, target, velocity, lifetime,
    wide_ref, out_ref, state_ref,
    weight_ref, index_ref, tiles, flat, occ_wide, occ_pad, window_ref, count_ref, mask_ref, chosen_ref, half_ref, term_ref, sems, small_sems,
):
    small = []
    for place, (origin, into) in enumerate((
        *((occ.at[v], occ_pad.at[pl.ds(v, 1)]) for v in range(MODES)),
        (count, count_ref),
        (window, window_ref),
        (velocity, state_ref.at[pl.ds(0, ROWS)]),
        (lifetime, state_ref.at[pl.ds(ROWS, BANDS)]),
        (source, index_ref.at[pl.ds(0, 1)]),
        (target, index_ref.at[pl.ds(1, 1)]),
    )):
        small.append(pltpu.make_async_copy(origin, into, small_sems.at[place]))
    for copy in small[:MODES]:
        copy.start()
    step = TILES // CHUNKS
    copies = []
    for c in range(CHUNKS):
        part = pl.ds(c * step, step)
        copies.append(pltpu.make_async_copy(coupling.at[part], tiles.at[part], sems.at[c]))
        copies[-1].start()
        if c == 0:
            for copy in small[MODES:]:
                copy.start()
    spread = (iota((16, LANES), 1) % MODES == iota((16, LANES), 0)).astype(F32).astype(BF16)
    gather = (iota((LANES, TILES), 0) // MODES == iota((LANES, TILES), 1) // 4).astype(F32).astype(BF16)
    group = iota((1, TILES), 1) % 4
    for copy in small[:MODES]:
        copy.wait()
    valid = iota((16, TILES), 0) < MODES
    occ_rows = jnp.where(valid, occ_pad[...], 0.0).T.astype(BF16)
    occ_wide[...] = jnp.dot(occ_rows, spread, preferred_element_type=F32)
    summed = None
    for c in range(CHUNKS + 1):
        before = summed
        if c < CHUNKS:
            copies[c].wait()
            rows = []
            for t in range(c * step, (c + 1) * step):
                tile = tiles[t]
                wide = jnp.broadcast_to(occ_wide[pl.ds(t, 1), :], (BANDS, LANES)).astype(BF16)
                rows.append(tile * tile * wide)
            summed = jnp.dot(jnp.concatenate(rows, axis=0), gather, preferred_element_type=F32)
        for t in range(step if c else 0):
            merged = before[t * BANDS : t * BANDS + 8, :]
            for j in range(1, 4):
                row = t * BANDS + j * 8
                merged = jnp.where(group == j, before[row : row + 8, :], merged)
            flat[pl.ds(((c - 1) * step + t) * 8, 8), :] = merged
    for copy in small[MODES:]:
        copy.wait()
    count = count_ref[...].astype(F32).astype(BF16)
    owner = (iota((64, TILES), 1) // TILE_SLOTS == iota((64, TILES), 0)).astype(F32).astype(BF16)
    live = jnp.dot(jnp.broadcast_to(count, (8, 64)), owner, preferred_element_type=F32)
    slot = (iota((8, TILES), 1) % TILE_SLOTS).astype(F32)
    live = (slot < live).astype(F32)
    mask = window_ref[...].astype(F32) * live[0:1, :]
    mask_ref[pl.ds(0, BANDS), :] = mask
    mask_ref[pl.ds(BANDS, BANDS), :] = mask
    for q in range(8):
        turned = flat[pl.ds(q, TILES, stride=8), :].T
        rows = mask_ref[pl.ds(q, 8, stride=8), :]
        for m in range(16):
            weight_ref[pl.ds(q * TILES + m * 8, 8), :] = turned[m * 8 : m * 8 + 8, :] * rows
    source_row = jnp.broadcast_to(index_ref[0:1, :], (16, TILES))
    wide_ref[pl.ds(0, WIDE), :] = weight_ref[...].astype(BF16)
    wide_ref[pl.ds(WIDE, 16), :] = source_row.astype(F32).astype(BF16)
    lifetime_now = state_ref[pl.ds(ROWS, BANDS), :]
    deviation = jnp.concatenate(
        [lifetime_now * state_ref[pl.ds(i * BANDS, BANDS), :] for i in range(3)], axis=0
    )
    picks = onehot(iota((TILES, TILES), 0) == index_ref[0:1, :])
    chosen_ref[...] = jnp.dot(deviation.astype(BF16), picks, preferred_element_type=F32)
    for i in range(3):
        band_terms(weight_ref, i * 64, band_pairs(chosen_ref, i), half_ref, term_ref, i)
    target = index_ref[1:2, :].astype(F32)
    term_ref[pl.ds(ROWS, BANDS), :] = jnp.where(iota((BANDS, TILES), 0) == 0, target, 0.0)
    out_ref[...] = term_ref[...].T.astype(BF16)


def receive_kernel(terms_ref, out_ref):
    terms = terms_ref[...].astype(F32)
    target = terms[:, ROWS : ROWS + 1].astype(jnp.int32)
    turned = terms.T
    places = onehot(iota((TILES, TILES), 1) == target)
    total = jnp.dot(turned[:ROWS, :].astype(BF16), places, preferred_element_type=F32)
    message = jnp.concatenate([total, turned[ROWS : ROWS + 8, :]], axis=0).astype(BF16)
    for p in range(out_ref.shape[0]):
        out_ref[p] = message


def direction_terms(deviation, weights, chosen_ref, half_ref, term_ref, out_ref):
    picks = []
    for weight in weights:
        source_row = weight[pl.ds(WIDE, 16), :].astype(F32)[0:1, :].astype(jnp.int32)
        picks.append(onehot(iota((TILES, TILES), 0) == source_row))
    chosen = jnp.dot(deviation.astype(BF16), jnp.concatenate(picks, axis=1), preferred_element_type=F32)
    for g, weight in enumerate(weights):
        chosen_ref[pl.ds(g * BANDS, BANDS), :] = chosen[:, g * TILES : (g + 1) * TILES]
    for g, weight in enumerate(weights):
        band_terms(weight, g * 64, band_pairs(chosen_ref, g), half_ref, term_ref, g)
    out_ref[...] = term_ref[...].T.astype(BF16)


def own_direction():
    return lax.axis_index("pb") // 2 % 3


def next_direction(state_ref, scattering):
    rows = pl.ds(pl.multiple_of(own_direction() * BANDS, BANDS), BANDS)
    return state_ref[pl.ds(ROWS, BANDS), :] * (state_ref[rows, :] + scattering)


def first_kernel(parts_ref, state_ref, w0, w1, w2, w3, out_ref, target_ref, chosen_ref, half_ref, term_ref):
    rows = pl.ds(pl.multiple_of(own_direction() * BANDS, BANDS), BANDS)
    total = parts_ref[0, rows, :].astype(F32)
    for p in range(1, parts_ref.shape[0]):
        total = total + parts_ref[p, rows, :].astype(F32)
    me = lax.axis_index("pb")
    groups = parts_ref.shape[0]
    for g in range(4):
        peer = lax.rem(me + groups - 2 * g, groups)
        target_ref[pl.ds(g, 1), :] = parts_ref[peer, pl.ds(ROWS, 8), :].astype(F32)[0:1, :]
    deviation = next_direction(state_ref, total)
    direction_terms(deviation, (w0, w1, w2, w3), chosen_ref, half_ref, term_ref, out_ref)


def step_kernel(mine_ref, other_ref, state_ref, w0, w1, w2, w3, out_ref, chosen_ref, half_ref, term_ref):
    deviation = next_direction(state_ref, mine_ref[...].astype(F32) + other_ref[...].astype(F32))
    direction_terms(deviation, (w0, w1, w2, w3), chosen_ref, half_ref, term_ref, out_ref)


def direction_sum(terms_ref, target_ref):
    turned = terms_ref[...].astype(F32).T.astype(BF16)
    left, right = [], []
    for g in range(4):
        target = target_ref[pl.ds(g, 1), :].astype(jnp.int32)
        right.append(onehot(iota((TILES, TILES), 0) == target))
        left.append(turned[g * BANDS : (g + 1) * BANDS, :])
    return lax.dot_general(
        jnp.concatenate(left, axis=1), jnp.concatenate(right, axis=1), (((1,), (1,)), ((), ())),
        preferred_element_type=F32,
    ).astype(BF16)


def sum_kernel(terms_ref, target_ref, out_ref):
    out_ref[...] = direction_sum(terms_ref, target_ref)


def last_sum_kernel(terms_ref, target_ref, out_ref):
    total = direction_sum(terms_ref, target_ref)
    for p in range(out_ref.shape[0]):
        out_ref[p] = total


def final_kernel(parts_ref, state_ref, out_ref):
    for i in range(3):
        total = parts_ref[2 * i].astype(F32) + parts_ref[2 * i + 1].astype(F32)
        rows = pl.ds(i * BANDS, BANDS)
        out_ref[rows, :] = state_ref[pl.ds(ROWS, BANDS), :] * (state_ref[rows, :] + total)


VMEM = pl.BlockSpec(memory_space=pltpu.VMEM)


def call(body, ins, outs, scratch=(), limit=4 << 20, flops=1000000):
    return pl.pallas_call(
        body,
        in_specs=ins,
        out_specs=[VMEM] * len(outs),
        out_shape=[jax.ShapeDtypeStruct(s, d) for s, d in outs],
        scratch_shapes=list(scratch),
        compiler_params=pltpu.CompilerParams(vmem_limit_bytes=limit),
        cost_estimate=pl.CostEstimate(flops=flops, bytes_accessed=1 << 20, transcendentals=0),
    )


def over_owners(terms):
    return lax.all_to_all(
        terms.reshape(-1, TILE_SLOTS, TILES), "ka", split_axis=0, concat_axis=0, tiled=True
    ).reshape(TILES, TILES)


def shards(coupling, phonon_occ, band_window, pair_count, k_target, kq_source, velocity, lifetime):
    groups = lax.axis_size("pb")
    small = [
        pltpu.VMEM((TILES, TILES), F32), pltpu.VMEM((4 * 64, TILES), F32), pltpu.VMEM((TILES, TILES), F32)
    ]
    wide, terms, state = call(
        weight_kernel, [pl.BlockSpec(memory_space=pltpu.HBM)] * 8,
        [((WIDE + 16, TILES), BF16), ((TILES, TILES), BF16), ((TILES, TILES), F32)],
        [
            pltpu.VMEM((WIDE, TILES), F32),
            pltpu.VMEM((8, TILES), jnp.int32),
            pltpu.VMEM((TILES, BANDS, LANES), BF16),
            pltpu.VMEM((TILES * 8, TILES), F32),
            pltpu.VMEM((TILES, LANES), F32),
            pltpu.VMEM((16, TILES), F32),
            pltpu.VMEM((BANDS, TILES), jnp.int32),
            pltpu.VMEM((1, 64), jnp.int32),
            pltpu.VMEM((2 * BANDS, TILES), F32),
            pltpu.VMEM((ROWS, TILES), F32), *small[1:],
            pltpu.SemaphoreType.DMA((CHUNKS,)),
            pltpu.SemaphoreType.DMA((MODES + 6,)),
        ],
        limit=16 << 20,
    )(*(pltpu.with_memory_space_constraint(x, pltpu.HBM) for x in (
        coupling[0, 0], phonon_occ.transpose(0, 3, 1, 2).reshape(MODES, 1, TILES), band_window[0, 0].T, pair_count[0],
        kq_source.reshape(1, TILES), k_target.reshape(1, TILES), velocity.reshape(ROWS, TILES), lifetime,
    )))
    arrived = over_owners(terms)
    weights = [wide]
    for shift in (1, 3, 2):
        weights.append(lax.ppermute(wide, "pb", [
            (p, (p + 2 * shift) % groups) for p in range(groups)
        ]))
    weights = [weights[0], weights[1], weights[3], weights[2]]
    (copies,) = call(receive_kernel, [VMEM], [((groups, ROWS + 8, TILES), BF16)])(arrived)
    parts = lax.all_to_all(copies, "pb", split_axis=0, concat_axis=0, tiled=True)
    terms, targets = call(
        first_kernel, [VMEM] * 6, [((TILES, TILES), BF16), ((8, TILES), F32)], small
    )(parts, state, *weights)
    for iteration in range(1, ITERS):
        if iteration > 1:
            other = lax.ppermute(mine, "pb", [(p, p + 1 - 2 * (p % 2)) for p in range(groups)])
            (terms,) = call(step_kernel, [VMEM] * 7, [((TILES, TILES), BF16)], small)(mine, other, state, *weights)
        arrived = over_owners(terms)
        if iteration < ITERS - 1:
            (mine,) = call(sum_kernel, [VMEM] * 2, [((BANDS, TILES), BF16)])(arrived, targets)
    (copies,) = call(last_sum_kernel, [VMEM] * 2, [((groups, BANDS, TILES), BF16)])(arrived, targets)
    parts = lax.all_to_all(copies, "pb", split_axis=0, concat_axis=0, tiled=True)
    (deviation,) = call(final_kernel, [VMEM] * 2, [((ROWS, TILES), F32)])(parts, state)
    return deviation.reshape(3, BANDS, TILES)


def solution(mesh):
    placed = (
        P("pb", "ka", None, None, None),
        P("pb", "ka", None, None),
        P("pb", "ka", None, None),
        P("pb", "ka", None),
        P("pb", "ka", None),
        P("pb", "ka", None),
        P(None, None, "ka"),
        P(None, "ka"),
    )
    return jax.shard_map(
        shards, mesh=mesh, in_specs=placed, out_specs=P(None, None, "ka"), check_vma=False
    )
```

```python
import jax
import jax.numpy as jnp
from jax import lax
from jax.experimental import pallas as pl
from jax.experimental.pallas import tpu as pltpu
from jax.sharding import PartitionSpec as P


MODES = 12
TILE_SLOTS = 2
BANDS = 32
ROWS = 3 * BANDS
TILES = 128
LANES = BANDS * MODES
CHUNKS = (16, 32, 40, 40)
PB = ("x", "core")
WIDE = BANDS * BANDS
F32 = jnp.float32
BF16 = jnp.bfloat16


def iota(shape, axis):
    return lax.broadcasted_iota(jnp.int32, shape, axis)


def band_terms(weight, base, pairs, half_ref, term_ref, slot):
    for q in range(8):
        total = None
        for m, pair in enumerate(pairs):
            term = weight[pl.ds(q * TILES + m * 8, 8), :].astype(F32) * pair
            total = term if total is None else total + term
        half_ref[pl.ds(base + q * 8, 8), :] = total
    for j in range(4):
        term_ref[pl.ds(slot * BANDS + j * 8, 8), :] = (
            half_ref[pl.ds(base + j, 8, stride=8), :] + half_ref[pl.ds(base + j + 4, 8, stride=8), :]
        )


def band_pairs(chosen_ref, slot):
    first = iota((8, TILES), 0) < 4
    pairs = []
    for m in range(0, BANDS, 2):
        row = slot * BANDS + m
        low = jnp.broadcast_to(chosen_ref[pl.ds(row, 1), :], (8, TILES))
        high = jnp.broadcast_to(chosen_ref[pl.ds(row + 1, 1), :], (8, TILES))
        pairs.append(jnp.where(first, low, high))
    return pairs


def onehot(equal):
    return equal.astype(F32).astype(BF16)


def weight_kernel(
    coupling, occ, window, count, source, target, velocity, lifetime,
    wide_ref, out_ref, state_ref,
    weight_ref, index_ref, tiles, flat, occ_wide, occ_pad, window_ref, count_ref, mask_ref, chosen_ref, half_ref, term_ref, sems, small_sems,
):
    small = []
    for place, (origin, into) in enumerate((
        *((occ.at[v], occ_pad.at[pl.ds(v, 1)]) for v in range(MODES)),
        (count, count_ref),
        (window, window_ref),
        (velocity, state_ref.at[pl.ds(0, ROWS)]),
        (lifetime, state_ref.at[pl.ds(ROWS, BANDS)]),
        (source, index_ref.at[pl.ds(0, 1)]),
        (target, index_ref.at[pl.ds(1, 1)]),
    )):
        small.append(pltpu.make_async_copy(origin, into, small_sems.at[place]))
    begin = [sum(CHUNKS[:c]) for c in range(len(CHUNKS))]
    copies = []
    for c, size in enumerate(CHUNKS):
        part = pl.ds(begin[c], size)
        copies.append(pltpu.make_async_copy(coupling.at[part], tiles.at[part], sems.at[c]))
        copies[-1].start()
        if c == 0:
            for copy in small[:MODES]:
                copy.start()
    for copy in small[MODES:]:
        copy.start()
    spread = (iota((16, LANES), 1) % MODES == iota((16, LANES), 0)).astype(F32).astype(BF16)
    gather = (iota((LANES, TILES), 0) // MODES == iota((LANES, TILES), 1) // 4).astype(F32).astype(BF16)
    group = iota((1, TILES), 1) % 4
    for copy in small[:MODES]:
        copy.wait()
    valid = iota((16, TILES), 0) < MODES
    occ_rows = jnp.where(valid, occ_pad[...], 0.0).T.astype(BF16)
    occ_wide[...] = jnp.dot(occ_rows, spread, preferred_element_type=F32)
    for c, size in enumerate(CHUNKS):
        copies[c].wait()
        rows = []
        for t in range(begin[c], begin[c] + size):
            tile = tiles[t]
            wide = jnp.broadcast_to(occ_wide[pl.ds(t, 1), :], (BANDS, LANES)).astype(BF16)
            rows.append(tile * tile * wide)
        summed = jnp.dot(jnp.concatenate(rows, axis=0), gather, preferred_element_type=F32)
        for t in range(size):
            merged = summed[t * BANDS : t * BANDS + 8, :]
            for j in range(1, 4):
                row = t * BANDS + j * 8
                merged = jnp.where(group == j, summed[row : row + 8, :], merged)
            flat[pl.ds((begin[c] + t) * 8, 8), :] = merged
    for copy in small[MODES:]:
        copy.wait()
    count = count_ref[...].astype(F32).astype(BF16)
    owner = (iota((64, TILES), 1) // TILE_SLOTS == iota((64, TILES), 0)).astype(F32).astype(BF16)
    live = jnp.dot(jnp.broadcast_to(count, (8, 64)), owner, preferred_element_type=F32)
    slot = (iota((8, TILES), 1) % TILE_SLOTS).astype(F32)
    live = (slot < live).astype(F32)
    mask = window_ref[...].astype(F32) * live[0:1, :]
    mask_ref[pl.ds(0, BANDS), :] = mask
    mask_ref[pl.ds(BANDS, BANDS), :] = mask
    for q in range(8):
        turned = flat[pl.ds(q, TILES, stride=8), :].T
        rows = mask_ref[pl.ds(q, 8, stride=8), :]
        for m in range(16):
            weight_ref[pl.ds(q * TILES + m * 8, 8), :] = turned[m * 8 : m * 8 + 8, :] * rows
    source_row = jnp.broadcast_to(index_ref[0:1, :], (16, TILES))
    wide_ref[pl.ds(0, WIDE), :] = weight_ref[...].astype(BF16)
    wide_ref[pl.ds(WIDE, 16), :] = source_row.astype(F32).astype(BF16)
    lifetime_now = state_ref[pl.ds(ROWS, BANDS), :]
    deviation = jnp.concatenate(
        [lifetime_now * state_ref[pl.ds(i * BANDS, BANDS), :] for i in range(3)], axis=0
    )
    picks = onehot(iota((TILES, TILES), 0) == index_ref[0:1, :])
    chosen_ref[...] = jnp.dot(deviation.astype(BF16), picks, preferred_element_type=F32)
    for i in range(3):
        band_terms(weight_ref, i * 64, band_pairs(chosen_ref, i), half_ref, term_ref, i)
    target = index_ref[1:2, :].astype(F32)
    term_ref[pl.ds(ROWS, BANDS), :] = jnp.where(iota((BANDS, TILES), 0) == 0, target, 0.0)
    out_ref[...] = term_ref[...].T.astype(BF16)


def receive_kernel(terms_ref, out_ref):
    terms = terms_ref[...].astype(F32)
    target = terms[:, ROWS : ROWS + 1].astype(jnp.int32)
    turned = terms.T
    places = onehot(iota((TILES, TILES), 1) == target)
    total = jnp.dot(turned[:ROWS, :].astype(BF16), places, preferred_element_type=F32)
    message = jnp.concatenate([total, turned[ROWS : ROWS + 8, :]], axis=0).astype(BF16)
    for p in range(out_ref.shape[0]):
        out_ref[p] = message


def direction_terms(deviation, weights, chosen_ref, half_ref, term_ref, out_ref):
    picks = []
    for weight in weights:
        source_row = weight[pl.ds(WIDE, 16), :].astype(F32)[0:1, :].astype(jnp.int32)
        picks.append(onehot(iota((TILES, TILES), 0) == source_row))
    chosen = jnp.dot(deviation.astype(BF16), jnp.concatenate(picks, axis=1), preferred_element_type=F32)
    for g, weight in enumerate(weights):
        chosen_ref[pl.ds(g * BANDS, BANDS), :] = chosen[:, g * TILES : (g + 1) * TILES]
    for g, weight in enumerate(weights):
        band_terms(weight, g * 64, band_pairs(chosen_ref, g), half_ref, term_ref, g)
    message = term_ref[...].T.astype(BF16)
    for core in range(out_ref.shape[0]):
        out_ref[core] = message


def own_direction():
    return lax.axis_index("x") % 3


def next_direction(state_ref, scattering):
    rows = pl.ds(pl.multiple_of(own_direction() * BANDS, BANDS), BANDS)
    return state_ref[pl.ds(ROWS, BANDS), :] * (state_ref[rows, :] + scattering)


def first_kernel(parts_ref, state_ref, w0, w1, w2, w3, out_ref, target_ref, chosen_ref, half_ref, term_ref):
    rows = pl.ds(pl.multiple_of(own_direction() * BANDS, BANDS), BANDS)
    total = parts_ref[0, rows, :].astype(F32)
    for p in range(1, parts_ref.shape[0]):
        total = total + parts_ref[p, rows, :].astype(F32)
    for g in range(4):
        for core in range(2):
            peer = 2 * jnp.bitwise_xor(lax.axis_index("x"), g) + core
            row = parts_ref[peer, pl.ds(ROWS, 8), :].astype(F32)[0:1, :]
            target_ref[pl.ds(2 * g + core, 1), :] = row
    deviation = next_direction(state_ref, total)
    direction_terms(deviation, (w0, w1, w2, w3), chosen_ref, half_ref, term_ref, out_ref)


def direction_sum(terms_ref, target_ref, cores):
    turned = terms_ref[...].astype(F32).T.astype(BF16)
    left, right = [], []
    for g in range(4):
        left.append(turned[g * BANDS : (g + 1) * BANDS, :])
        for core in cores:
            target = target_ref[pl.ds(2 * g + core, 1), :].astype(jnp.int32)
            right.append(onehot(iota((TILES, TILES), 0) == target))
    return lax.dot_general(
        jnp.concatenate(left, axis=1), jnp.concatenate(right, axis=1), (((1,), (1,)), ((), ())),
        preferred_element_type=F32,
    )


def step_kernel(terms_ref, target_ref, state_ref, w0, w1, w2, w3, out_ref, chosen_ref, half_ref, term_ref):
    deviation = next_direction(state_ref, direction_sum(terms_ref, target_ref, (0, 1)))
    direction_terms(deviation, (w0, w1, w2, w3), chosen_ref, half_ref, term_ref, out_ref)


def last_kernel(terms_ref, target_ref, out_ref):
    total = direction_sum(terms_ref, target_ref, (lax.axis_index("core"),)).astype(BF16)
    for p in range(out_ref.shape[0]):
        out_ref[p] = total


def final_kernel(parts_ref, state_ref, out_ref):
    for i in range(3):
        total = parts_ref[2 * i].astype(F32) + parts_ref[2 * i + 1].astype(F32)
        rows = pl.ds(i * BANDS, BANDS)
        out_ref[rows, :] = state_ref[pl.ds(ROWS, BANDS), :] * (state_ref[rows, :] + total)


VMEM = pl.BlockSpec(memory_space=pltpu.VMEM)


def call(body, ins, outs, scratch=(), limit=4 << 20, flops=1000000):
    return pl.pallas_call(
        body,
        in_specs=ins,
        out_specs=[VMEM] * len(outs),
        out_shape=[jax.ShapeDtypeStruct(s, d) for s, d in outs],
        scratch_shapes=list(scratch),
        compiler_params=pltpu.CompilerParams(vmem_limit_bytes=limit),
        cost_estimate=pl.CostEstimate(flops=flops, bytes_accessed=1 << 20, transcendentals=0),
    )


def over_owners(terms, axes):
    return lax.all_to_all(
        terms.reshape(-1, TILE_SLOTS, TILES), axes, split_axis=0, concat_axis=0, tiled=True
    ).reshape(-1, TILES)


def shards(coupling, phonon_occ, band_window, pair_count, k_target, kq_source, velocity, lifetime):
    groups = lax.axis_size("x") * lax.axis_size("core")
    small = [
        pltpu.VMEM((TILES, TILES), F32), pltpu.VMEM((4 * 64, TILES), F32), pltpu.VMEM((TILES, TILES), F32)
    ]
    wide, terms, state = call(
        weight_kernel, [pl.BlockSpec(memory_space=pltpu.HBM)] * 8,
        [((WIDE + 16, TILES), BF16), ((TILES, TILES), BF16), ((TILES, TILES), F32)],
        [
            pltpu.VMEM((WIDE, TILES), F32),
            pltpu.VMEM((8, TILES), jnp.int32),
            pltpu.VMEM((TILES, BANDS, LANES), BF16),
            pltpu.VMEM((TILES * 8, TILES), F32),
            pltpu.VMEM((TILES, LANES), F32),
            pltpu.VMEM((16, TILES), F32),
            pltpu.VMEM((BANDS, TILES), jnp.int32),
            pltpu.VMEM((1, 64), jnp.int32),
            pltpu.VMEM((2 * BANDS, TILES), F32),
            pltpu.VMEM((ROWS, TILES), F32), *small[1:],
            pltpu.SemaphoreType.DMA((len(CHUNKS),)),
            pltpu.SemaphoreType.DMA((MODES + 6,)),
        ],
        limit=16 << 20,
    )(*(pltpu.with_memory_space_constraint(x, pltpu.HBM) for x in (
        coupling[0, 0], phonon_occ.transpose(0, 3, 1, 2).reshape(MODES, 1, TILES), band_window[0, 0].T, pair_count[0],
        kq_source.reshape(1, TILES), k_target.reshape(1, TILES), velocity.reshape(ROWS, TILES), lifetime,
    )))
    arrived = over_owners(terms, "ka")
    weights = [wide]
    for flip in (2, 4, 6):
        weights.append(lax.ppermute(wide, PB, [(p, p ^ flip) for p in range(groups) if p ^ flip < 6]))
    (copies,) = call(receive_kernel, [VMEM], [((groups, ROWS + 8, TILES), BF16)])(arrived)
    parts = lax.all_to_all(copies, PB, split_axis=0, concat_axis=0, tiled=True)
    terms, targets = call(
        first_kernel, [VMEM] * 6, [((2, TILES, TILES), BF16), ((8, TILES), F32)], small
    )(parts, state, *weights)
    for copied in (2, 1):
        arrived = over_owners(terms, ("core", "ka"))
        (terms,) = call(step_kernel, [VMEM] * 7, [((copied, TILES, TILES), BF16)], small)(
            arrived, targets, state, *weights
        )
    arrived = over_owners(terms, "ka")
    (copies,) = call(last_kernel, [VMEM] * 2, [((groups, BANDS, TILES), BF16)])(arrived, targets)
    parts = lax.all_to_all(copies, PB, split_axis=0, concat_axis=0, tiled=True)
    (deviation,) = call(final_kernel, [VMEM] * 2, [((ROWS, TILES), F32)])(parts, state)
    return deviation.reshape(3, BANDS, TILES)


def solution(mesh):
    fine = jax.sharding.Mesh(mesh.devices.reshape(4, 2, -1), (*PB, "ka"))
    placed = (
        P(PB, "ka", None, None, None),
        P(PB, "ka", None, None),
        P(PB, "ka", None, None),
        P(PB, "ka", None),
        P(PB, "ka", None),
        P(PB, "ka", None),
        P(None, None, "ka"),
        P(None, "ka"),
    )
    return jax.shard_map(
        shards, mesh=fine, in_specs=placed, out_specs=P(None, None, "ka"), check_vma=False
    )
```

```python
import jax
import jax.numpy as jnp
from jax import lax
from jax.experimental import pallas as pl
from jax.experimental.pallas import tpu as pltpu
from jax.sharding import PartitionSpec as P


MODES = 12
TILE_SLOTS = 2
BANDS = 32
ROWS = 3 * BANDS
TILES = 128
LANES = BANDS * MODES
CHUNKS = (24, 48, 56)
PB = ("x", "core")
WIDE = BANDS * BANDS
F32 = jnp.float32
BF16 = jnp.bfloat16


def iota(shape, axis):
    return lax.broadcasted_iota(jnp.int32, shape, axis)


def band_terms(weight, base, pairs, half_ref, term_ref, slot):
    for q in range(8):
        total = None
        for m, pair in enumerate(pairs):
            term = weight[pl.ds(q * TILES + m * 8, 8), :].astype(F32) * pair
            total = term if total is None else total + term
        half_ref[pl.ds(base + q * 8, 8), :] = total
    for j in range(4):
        term_ref[pl.ds(slot * BANDS + j * 8, 8), :] = (
            half_ref[pl.ds(base + j, 8, stride=8), :] + half_ref[pl.ds(base + j + 4, 8, stride=8), :]
        )


def band_pairs(chosen_ref, slot):
    first = iota((8, TILES), 0) < 4
    pairs = []
    for m in range(0, BANDS, 2):
        row = slot * BANDS + m
        low = jnp.broadcast_to(chosen_ref[pl.ds(row, 1), :], (8, TILES))
        high = jnp.broadcast_to(chosen_ref[pl.ds(row + 1, 1), :], (8, TILES))
        pairs.append(jnp.where(first, low, high))
    return pairs


def onehot(equal):
    return equal.astype(F32).astype(BF16)


def weight_kernel(
    coupling, occ, window, count, source, target, velocity, lifetime,
    wide_ref, out_ref, state_ref,
    weight_ref, index_ref, tiles, flat, occ_wide, occ_pad, window_ref, count_ref, mask_ref, chosen_ref, half_ref, term_ref, sems, small_sems,
):
    small = []
    for place, (origin, into) in enumerate((
        *((occ.at[v], occ_pad.at[pl.ds(v, 1)]) for v in range(MODES)),
        (count, count_ref),
        (window, window_ref),
        (velocity, state_ref.at[pl.ds(0, ROWS)]),
        (lifetime, state_ref.at[pl.ds(ROWS, BANDS)]),
        (source, index_ref.at[pl.ds(0, 1)]),
        (target, index_ref.at[pl.ds(1, 1)]),
    )):
        small.append(pltpu.make_async_copy(origin, into, small_sems.at[place]))
    begin = [sum(CHUNKS[:c]) for c in range(len(CHUNKS))]
    copies = []
    for c, size in enumerate(CHUNKS):
        part = pl.ds(begin[c], size)
        copies.append(pltpu.make_async_copy(coupling.at[part], tiles.at[part], sems.at[c]))
        copies[-1].start()
        if c == 0:
            for copy in small[:MODES]:
                copy.start()
    for copy in small[MODES:]:
        copy.start()
    spread = (iota((16, LANES), 1) % MODES == iota((16, LANES), 0)).astype(F32).astype(BF16)
    gather = (iota((LANES, TILES), 0) // MODES == iota((LANES, TILES), 1) // 4).astype(F32).astype(BF16)
    group = iota((1, TILES), 1) % 4
    for copy in small[:MODES]:
        copy.wait()
    valid = iota((16, TILES), 0) < MODES
    occ_rows = jnp.where(valid, occ_pad[...], 0.0).T.astype(BF16)
    occ_wide[...] = jnp.dot(occ_rows, spread, preferred_element_type=F32)
    for c, size in enumerate(CHUNKS):
        copies[c].wait()
        rows = []
        for t in range(begin[c], begin[c] + size):
            tile = tiles[t]
            wide = jnp.broadcast_to(occ_wide[pl.ds(t, 1), :], (BANDS, LANES)).astype(BF16)
            rows.append(tile * tile * wide)
        summed = jnp.dot(jnp.concatenate(rows, axis=0), gather, preferred_element_type=F32)
        for t in range(size):
            merged = summed[t * BANDS : t * BANDS + 8, :]
            for j in range(1, 4):
                row = t * BANDS + j * 8
                merged = jnp.where(group == j, summed[row : row + 8, :], merged)
            flat[pl.ds((begin[c] + t) * 8, 8), :] = merged
    for copy in small[MODES:]:
        copy.wait()
    count = count_ref[...].astype(F32).astype(BF16)
    owner = (iota((64, TILES), 1) // TILE_SLOTS == iota((64, TILES), 0)).astype(F32).astype(BF16)
    live = jnp.dot(jnp.broadcast_to(count, (8, 64)), owner, preferred_element_type=F32)
    slot = (iota((8, TILES), 1) % TILE_SLOTS).astype(F32)
    live = (slot < live).astype(F32)
    mask = window_ref[...].astype(F32) * live[0:1, :]
    mask_ref[pl.ds(0, BANDS), :] = mask
    mask_ref[pl.ds(BANDS, BANDS), :] = mask
    for q in range(8):
        turned = flat[pl.ds(q, TILES, stride=8), :].T
        rows = mask_ref[pl.ds(q, 8, stride=8), :]
        for m in range(16):
            weight_ref[pl.ds(q * TILES + m * 8, 8), :] = turned[m * 8 : m * 8 + 8, :] * rows
    source_row = jnp.broadcast_to(index_ref[0:1, :], (16, TILES))
    wide_ref[pl.ds(0, WIDE), :] = weight_ref[...].astype(BF16)
    wide_ref[pl.ds(WIDE, 16), :] = source_row.astype(F32).astype(BF16)
    lifetime_now = state_ref[pl.ds(ROWS, BANDS), :]
    deviation = jnp.concatenate(
        [lifetime_now * state_ref[pl.ds(i * BANDS, BANDS), :] for i in range(3)], axis=0
    )
    picks = onehot(iota((TILES, TILES), 0) == index_ref[0:1, :])
    chosen_ref[...] = jnp.dot(deviation.astype(BF16), picks, preferred_element_type=F32)
    for i in range(3):
        band_terms(weight_ref, i * 64, band_pairs(chosen_ref, i), half_ref, term_ref, i)
    target = index_ref[1:2, :].astype(F32)
    term_ref[pl.ds(ROWS, BANDS), :] = jnp.where(iota((BANDS, TILES), 0) == 0, target, 0.0)
    out_ref[...] = term_ref[...].T.astype(BF16)


def receive_kernel(terms_ref, out_ref):
    terms = terms_ref[...].astype(F32)
    target = terms[:, ROWS : ROWS + 1].astype(jnp.int32)
    turned = terms.T
    places = onehot(iota((TILES, TILES), 1) == target)
    total = jnp.dot(turned[:ROWS, :].astype(BF16), places, preferred_element_type=F32)
    targets = turned[ROWS : ROWS + 8, :]
    messages = [
        jnp.concatenate([total[i * BANDS : (i + 1) * BANDS, :], targets], axis=0).astype(BF16)
        for i in range(3)
    ]
    for p in range(out_ref.shape[0]):
        out_ref[p] = messages[p // 2 % 3]


def direction_terms(deviation, weights, chosen_ref, half_ref, term_ref, out_ref):
    picks = []
    for weight in weights:
        source_row = weight[pl.ds(WIDE, 16), :].astype(F32)[0:1, :].astype(jnp.int32)
        picks.append(onehot(iota((TILES, TILES), 0) == source_row))
    chosen = jnp.dot(deviation.astype(BF16), jnp.concatenate(picks, axis=1), preferred_element_type=F32)
    for g, weight in enumerate(weights):
        chosen_ref[pl.ds(g * BANDS, BANDS), :] = chosen[:, g * TILES : (g + 1) * TILES]
    for g, weight in enumerate(weights):
        band_terms(weight, g * 64, band_pairs(chosen_ref, g), half_ref, term_ref, g)
    message = term_ref[...].T.astype(BF16)
    for core in range(out_ref.shape[0]):
        out_ref[core] = message


def own_direction():
    return lax.axis_index("x") % 3


def next_direction(state_ref, scattering):
    rows = pl.ds(pl.multiple_of(own_direction() * BANDS, BANDS), BANDS)
    return state_ref[pl.ds(ROWS, BANDS), :] * (state_ref[rows, :] + scattering)


def first_kernel(parts_ref, state_ref, w0, w1, w2, w3, out_ref, target_ref, chosen_ref, half_ref, term_ref):
    total = parts_ref[0, pl.ds(0, BANDS), :].astype(F32)
    for p in range(1, parts_ref.shape[0]):
        total = total + parts_ref[p, pl.ds(0, BANDS), :].astype(F32)
    for g in range(4):
        for core in range(2):
            peer = 2 * jnp.bitwise_xor(lax.axis_index("x"), g) + core
            row = parts_ref[peer, pl.ds(BANDS, 8), :].astype(F32)[0:1, :]
            target_ref[pl.ds(2 * g + core, 1), :] = row
    deviation = next_direction(state_ref, total)
    direction_terms(deviation, (w0, w1, w2, w3), chosen_ref, half_ref, term_ref, out_ref)


def direction_sum(terms_ref, target_ref, cores):
    turned = terms_ref[...].astype(F32).T.astype(BF16)
    left, right = [], []
    for g in range(4):
        left.append(turned[g * BANDS : (g + 1) * BANDS, :])
        for core in cores:
            target = target_ref[pl.ds(2 * g + core, 1), :].astype(jnp.int32)
            right.append(onehot(iota((TILES, TILES), 0) == target))
    return lax.dot_general(
        jnp.concatenate(left, axis=1), jnp.concatenate(right, axis=1), (((1,), (1,)), ((), ())),
        preferred_element_type=F32,
    )


def step_kernel(terms_ref, target_ref, state_ref, w0, w1, w2, w3, out_ref, chosen_ref, half_ref, term_ref):
    deviation = next_direction(state_ref, direction_sum(terms_ref, target_ref, (0, 1)))
    direction_terms(deviation, (w0, w1, w2, w3), chosen_ref, half_ref, term_ref, out_ref)


def last_kernel(terms_ref, target_ref, out_ref):
    total = direction_sum(terms_ref, target_ref, (lax.axis_index("core"),)).astype(BF16)
    for p in range(out_ref.shape[0]):
        out_ref[p] = total


def final_kernel(parts_ref, state_ref, out_ref):
    for i in range(3):
        total = parts_ref[2 * i].astype(F32) + parts_ref[2 * i + 1].astype(F32)
        rows = pl.ds(i * BANDS, BANDS)
        out_ref[rows, :] = state_ref[pl.ds(ROWS, BANDS), :] * (state_ref[rows, :] + total)


VMEM = pl.BlockSpec(memory_space=pltpu.VMEM)


def call(body, ins, outs, scratch=(), limit=4 << 20, flops=1000000):
    return pl.pallas_call(
        body,
        in_specs=ins,
        out_specs=[VMEM] * len(outs),
        out_shape=[jax.ShapeDtypeStruct(s, d) for s, d in outs],
        scratch_shapes=list(scratch),
        compiler_params=pltpu.CompilerParams(vmem_limit_bytes=limit),
        cost_estimate=pl.CostEstimate(flops=flops, bytes_accessed=1 << 20, transcendentals=0),
    )


def over_owners(terms, axes):
    return lax.all_to_all(
        terms.reshape(-1, TILE_SLOTS, TILES), axes, split_axis=0, concat_axis=0, tiled=True
    ).reshape(-1, TILES)


def shards(coupling, phonon_occ, band_window, pair_count, k_target, kq_source, velocity, lifetime):
    groups = lax.axis_size("x") * lax.axis_size("core")
    small = [
        pltpu.VMEM((TILES, TILES), F32), pltpu.VMEM((4 * 64, TILES), F32), pltpu.VMEM((TILES, TILES), F32)
    ]
    wide, terms, state = call(
        weight_kernel, [pl.BlockSpec(memory_space=pltpu.HBM)] * 8,
        [((WIDE + 16, TILES), BF16), ((TILES, TILES), BF16), ((TILES, TILES), F32)],
        [
            pltpu.VMEM((WIDE, TILES), F32),
            pltpu.VMEM((8, TILES), jnp.int32),
            pltpu.VMEM((TILES, BANDS, LANES), BF16),
            pltpu.VMEM((TILES * 8, TILES), F32),
            pltpu.VMEM((TILES, LANES), F32),
            pltpu.VMEM((16, TILES), F32),
            pltpu.VMEM((BANDS, TILES), jnp.int32),
            pltpu.VMEM((1, 64), jnp.int32),
            pltpu.VMEM((2 * BANDS, TILES), F32),
            pltpu.VMEM((ROWS, TILES), F32), *small[1:],
            pltpu.SemaphoreType.DMA((len(CHUNKS),)),
            pltpu.SemaphoreType.DMA((MODES + 6,)),
        ],
        limit=16 << 20,
    )(*(pltpu.with_memory_space_constraint(x, pltpu.HBM) for x in (
        coupling[0, 0], phonon_occ.transpose(0, 3, 1, 2).reshape(MODES, 1, TILES), band_window[0, 0].T, pair_count[0],
        kq_source.reshape(1, TILES), k_target.reshape(1, TILES), velocity.reshape(ROWS, TILES), lifetime,
    )))
    arrived = over_owners(terms, "ka")
    weights = [wide]
    for flip in (2, 4, 6):
        weights.append(lax.ppermute(wide, PB, [(p, p ^ flip) for p in range(groups) if p ^ flip < 6]))
    (copies,) = call(receive_kernel, [VMEM], [((groups, BANDS + 8, TILES), BF16)])(arrived)
    parts = lax.all_to_all(copies, PB, split_axis=0, concat_axis=0, tiled=True)
    terms, targets = call(
        first_kernel, [VMEM] * 6, [((2, TILES, TILES), BF16), ((8, TILES), F32)], small
    )(parts, state, *weights)
    for copied in (2, 1):
        arrived = over_owners(terms, ("core", "ka"))
        (terms,) = call(step_kernel, [VMEM] * 7, [((copied, TILES, TILES), BF16)], small)(
            arrived, targets, state, *weights
        )
    arrived = over_owners(terms, "ka")
    (copies,) = call(last_kernel, [VMEM] * 2, [((groups, BANDS, TILES), BF16)])(arrived, targets)
    parts = lax.all_to_all(copies, PB, split_axis=0, concat_axis=0, tiled=True)
    (deviation,) = call(final_kernel, [VMEM] * 2, [((ROWS, TILES), F32)])(parts, state)
    return deviation.reshape(3, BANDS, TILES)


def solution(mesh):
    fine = jax.sharding.Mesh(mesh.devices.reshape(4, 2, -1), (*PB, "ka"))
    placed = (
        P(PB, "ka", None, None, None),
        P(PB, "ka", None, None),
        P(PB, "ka", None, None),
        P(PB, "ka", None),
        P(PB, "ka", None),
        P(PB, "ka", None),
        P(None, None, "ka"),
        P(None, "ka"),
    )
    return jax.shard_map(
        shards, mesh=fine, in_specs=placed, out_specs=P(None, None, "ka"), check_vma=False
    )
```

```python
import jax
import jax.numpy as jnp
from jax import lax
from jax.experimental import pallas as pl
from jax.experimental.pallas import tpu as pltpu
from jax.sharding import PartitionSpec as P


MODES = 12
TILE_SLOTS = 2
BANDS = 32
ROWS = 3 * BANDS
TILES = 128
LANES = BANDS * MODES
CHUNKS = (24, 48, 56)
PB = ("x", "core")
WIDE = BANDS * BANDS
F32 = jnp.float32
BF16 = jnp.bfloat16


def iota(shape, axis):
    return lax.broadcasted_iota(jnp.int32, shape, axis)


def band_terms(weight, base, pairs, half_ref, term_ref, slot):
    for q in range(8):
        total = None
        for m, pair in enumerate(pairs):
            term = weight[pl.ds(q * TILES + m * 8, 8), :].astype(F32) * pair
            total = term if total is None else total + term
        half_ref[pl.ds(base + q * 8, 8), :] = total
    for j in range(4):
        term_ref[pl.ds(slot * BANDS + j * 8, 8), :] = (
            half_ref[pl.ds(base + j, 8, stride=8), :] + half_ref[pl.ds(base + j + 4, 8, stride=8), :]
        )


def band_pairs(chosen_ref, slot):
    first = iota((8, TILES), 0) < 4
    pairs = []
    for m in range(0, BANDS, 2):
        row = slot * BANDS + m
        low = jnp.broadcast_to(chosen_ref[pl.ds(row, 1), :], (8, TILES))
        high = jnp.broadcast_to(chosen_ref[pl.ds(row + 1, 1), :], (8, TILES))
        pairs.append(jnp.where(first, low, high))
    return pairs


def onehot(equal):
    return equal.astype(F32).astype(BF16)


def weight_kernel(
    coupling, occ, window, count, source, target, velocity, lifetime,
    wide_ref, out_ref, state_ref,
    weight_ref, index_ref, tiles, flat, occ_wide, occ_pad, window_ref, count_ref, mask_ref, chosen_ref, half_ref, term_ref, sems, small_sems,
):
    small = []
    for place, (origin, into) in enumerate((
        *((occ.at[v], occ_pad.at[pl.ds(v, 1)]) for v in range(MODES)),
        (count, count_ref),
        (window, window_ref),
        (velocity, state_ref.at[pl.ds(0, ROWS)]),
        (lifetime, state_ref.at[pl.ds(ROWS, BANDS)]),
        (source, index_ref.at[pl.ds(0, 1)]),
        (target, index_ref.at[pl.ds(1, 1)]),
    )):
        small.append(pltpu.make_async_copy(origin, into, small_sems.at[place]))
    begin = [sum(CHUNKS[:c]) for c in range(len(CHUNKS))]
    copies = []
    for c, size in enumerate(CHUNKS):
        part = pl.ds(begin[c], size)
        copies.append(pltpu.make_async_copy(coupling.at[part], tiles.at[part], sems.at[c]))
        copies[-1].start()
        if c == 0:
            for copy in small[:MODES]:
                copy.start()
    for copy in small[MODES:]:
        copy.start()
    spread = (iota((16, LANES), 1) % MODES == iota((16, LANES), 0)).astype(F32).astype(BF16)
    gather = (iota((LANES, TILES), 0) // MODES == iota((LANES, TILES), 1) // 4).astype(F32).astype(BF16)
    group = iota((1, TILES), 1) % 4
    for copy in small[:MODES]:
        copy.wait()
    valid = iota((16, TILES), 0) < MODES
    occ_rows = jnp.where(valid, occ_pad[...], 0.0).T.astype(BF16)
    occ_wide[...] = jnp.dot(occ_rows, spread, preferred_element_type=F32)
    for c, size in enumerate(CHUNKS):
        copies[c].wait()
        rows = []
        for t in range(begin[c], begin[c] + size):
            tile = tiles[t]
            wide = jnp.broadcast_to(occ_wide[pl.ds(t, 1), :], (BANDS, LANES)).astype(BF16)
            rows.append(tile * tile * wide)
        summed = jnp.dot(jnp.concatenate(rows, axis=0), gather, preferred_element_type=F32)
        for t in range(size):
            merged = summed[t * BANDS : t * BANDS + 8, :]
            for j in range(1, 4):
                row = t * BANDS + j * 8
                merged = jnp.where(group == j, summed[row : row + 8, :], merged)
            flat[pl.ds((begin[c] + t) * 8, 8), :] = merged
    for copy in small[MODES:]:
        copy.wait()
    count = count_ref[...].astype(F32).astype(BF16)
    owner = (iota((64, TILES), 1) // TILE_SLOTS == iota((64, TILES), 0)).astype(F32).astype(BF16)
    live = jnp.dot(jnp.broadcast_to(count, (8, 64)), owner, preferred_element_type=F32)
    slot = (iota((8, TILES), 1) % TILE_SLOTS).astype(F32)
    live = (slot < live).astype(F32)
    mask = window_ref[...].astype(F32) * live[0:1, :]
    mask_ref[pl.ds(0, BANDS), :] = mask
    mask_ref[pl.ds(BANDS, BANDS), :] = mask
    for q in range(8):
        turned = flat[pl.ds(q, TILES, stride=8), :].T
        rows = mask_ref[pl.ds(q, 8, stride=8), :]
        for m in range(16):
            weight_ref[pl.ds(q * TILES + m * 8, 8), :] = turned[m * 8 : m * 8 + 8, :] * rows
    source_row = jnp.broadcast_to(index_ref[0:1, :], (16, TILES))
    wide_ref[pl.ds(0, WIDE), :] = weight_ref[...].astype(BF16)
    wide_ref[pl.ds(WIDE, 16), :] = source_row.astype(F32).astype(BF16)
    lifetime_now = state_ref[pl.ds(ROWS, BANDS), :]
    deviation = jnp.concatenate(
        [lifetime_now * state_ref[pl.ds(i * BANDS, BANDS), :] for i in range(3)], axis=0
    )
    picks = onehot(iota((TILES, TILES), 0) == index_ref[0:1, :])
    chosen_ref[...] = jnp.dot(deviation.astype(BF16), picks, preferred_element_type=F32)
    for i in range(3):
        band_terms(weight_ref, i * 64, band_pairs(chosen_ref, i), half_ref, term_ref, i)
    target = index_ref[1:2, :].astype(F32)
    term_ref[pl.ds(ROWS, BANDS), :] = jnp.where(iota((BANDS, TILES), 0) == 0, target, 0.0)
    out_ref[...] = term_ref[...].T.astype(BF16)


def receive_kernel(terms_ref, out_ref):
    terms = terms_ref[...].astype(F32)
    target = terms[:, ROWS : ROWS + 1].astype(jnp.int32)
    turned = terms.T
    places = onehot(iota((TILES, TILES), 1) == target)
    total = jnp.dot(turned[:ROWS, :].astype(BF16), places, preferred_element_type=F32)
    targets = turned[ROWS : ROWS + 8, :]
    messages = [
        jnp.concatenate([total[i * BANDS : (i + 1) * BANDS, :], targets], axis=0).astype(BF16)
        for i in range(3)
    ]
    for p in range(out_ref.shape[0]):
        out_ref[p] = messages[p // 2 % 3]


def direction_terms(deviation, weights, chosen_ref, half_ref, term_ref, out_ref):
    picks = []
    for weight in weights:
        source_row = weight[pl.ds(WIDE, 16), :].astype(F32)[0:1, :].astype(jnp.int32)
        picks.append(onehot(iota((TILES, TILES), 0) == source_row))
    chosen = jnp.dot(deviation.astype(BF16), jnp.concatenate(picks, axis=1), preferred_element_type=F32)
    for g, weight in enumerate(weights):
        chosen_ref[pl.ds(g * BANDS, BANDS), :] = chosen[:, g * TILES : (g + 1) * TILES]
    for g, weight in enumerate(weights):
        band_terms(weight, g * 64, band_pairs(chosen_ref, g), half_ref, term_ref, g)
    message = term_ref[...].T.astype(BF16)
    for core in range(out_ref.shape[0]):
        out_ref[core] = message


def own_direction():
    return lax.axis_index("x") % 3


def next_direction(state_ref, scattering):
    rows = pl.ds(pl.multiple_of(own_direction() * BANDS, BANDS), BANDS)
    return state_ref[pl.ds(ROWS, BANDS), :] * (state_ref[rows, :] + scattering)


def first_kernel(parts_ref, state_ref, w0, w1, w2, w3, out_ref, target_ref, chosen_ref, half_ref, term_ref):
    total = parts_ref[0, pl.ds(0, BANDS), :].astype(F32)
    for p in range(1, parts_ref.shape[0]):
        total = total + parts_ref[p, pl.ds(0, BANDS), :].astype(F32)
    for g in range(4):
        for core in range(2):
            peer = 2 * lax.rem(lax.axis_index("x") + 4 - g, 4) + core
            row = parts_ref[peer, pl.ds(BANDS, 8), :].astype(F32)[0:1, :]
            target_ref[pl.ds(2 * g + core, 1), :] = row
    deviation = next_direction(state_ref, total)
    direction_terms(deviation, (w0, w1, w2, w3), chosen_ref, half_ref, term_ref, out_ref)


def direction_sum(terms_ref, target_ref, cores):
    turned = terms_ref[...].astype(F32).T.astype(BF16)
    left, right = [], []
    for g in range(4):
        left.append(turned[g * BANDS : (g + 1) * BANDS, :])
        for core in cores:
            target = target_ref[pl.ds(2 * g + core, 1), :].astype(jnp.int32)
            right.append(onehot(iota((TILES, TILES), 0) == target))
    return lax.dot_general(
        jnp.concatenate(left, axis=1), jnp.concatenate(right, axis=1), (((1,), (1,)), ((), ())),
        preferred_element_type=F32,
    )


def step_kernel(terms_ref, target_ref, state_ref, w0, w1, w2, w3, out_ref, chosen_ref, half_ref, term_ref):
    deviation = next_direction(state_ref, direction_sum(terms_ref, target_ref, (0, 1)))
    direction_terms(deviation, (w0, w1, w2, w3), chosen_ref, half_ref, term_ref, out_ref)


def last_kernel(terms_ref, target_ref, out_ref):
    total = direction_sum(terms_ref, target_ref, (lax.axis_index("core"),)).astype(BF16)
    for p in range(out_ref.shape[0]):
        out_ref[p] = total


def final_kernel(parts_ref, state_ref, out_ref):
    for i in range(3):
        total = parts_ref[2 * i].astype(F32) + parts_ref[2 * i + 1].astype(F32)
        rows = pl.ds(i * BANDS, BANDS)
        out_ref[rows, :] = state_ref[pl.ds(ROWS, BANDS), :] * (state_ref[rows, :] + total)


VMEM = pl.BlockSpec(memory_space=pltpu.VMEM)


def call(body, ins, outs, scratch=(), limit=4 << 20, flops=1000000):
    return pl.pallas_call(
        body,
        in_specs=ins,
        out_specs=[VMEM] * len(outs),
        out_shape=[jax.ShapeDtypeStruct(s, d) for s, d in outs],
        scratch_shapes=list(scratch),
        compiler_params=pltpu.CompilerParams(vmem_limit_bytes=limit),
        cost_estimate=pl.CostEstimate(flops=flops, bytes_accessed=1 << 20, transcendentals=0),
    )


def over_owners(terms, axes):
    return lax.all_to_all(
        terms.reshape(-1, TILE_SLOTS, TILES), axes, split_axis=0, concat_axis=0, tiled=True
    ).reshape(-1, TILES)


def shards(coupling, phonon_occ, band_window, pair_count, k_target, kq_source, velocity, lifetime):
    groups = lax.axis_size("x") * lax.axis_size("core")
    small = [
        pltpu.VMEM((TILES, TILES), F32), pltpu.VMEM((4 * 64, TILES), F32), pltpu.VMEM((TILES, TILES), F32)
    ]
    wide, terms, state = call(
        weight_kernel, [pl.BlockSpec(memory_space=pltpu.HBM)] * 8,
        [((WIDE + 16, TILES), BF16), ((TILES, TILES), BF16), ((TILES, TILES), F32)],
        [
            pltpu.VMEM((WIDE, TILES), F32),
            pltpu.VMEM((8, TILES), jnp.int32),
            pltpu.VMEM((TILES, BANDS, LANES), BF16),
            pltpu.VMEM((TILES * 8, TILES), F32),
            pltpu.VMEM((TILES, LANES), F32),
            pltpu.VMEM((16, TILES), F32),
            pltpu.VMEM((BANDS, TILES), jnp.int32),
            pltpu.VMEM((1, 64), jnp.int32),
            pltpu.VMEM((2 * BANDS, TILES), F32),
            pltpu.VMEM((ROWS, TILES), F32), *small[1:],
            pltpu.SemaphoreType.DMA((len(CHUNKS),)),
            pltpu.SemaphoreType.DMA((MODES + 6,)),
        ],
        limit=16 << 20,
    )(*(pltpu.with_memory_space_constraint(x, pltpu.HBM) for x in (
        coupling[0, 0], phonon_occ.transpose(0, 3, 1, 2).reshape(MODES, 1, TILES), band_window[0, 0].T, pair_count[0],
        kq_source.reshape(1, TILES), k_target.reshape(1, TILES), velocity.reshape(ROWS, TILES), lifetime,
    )))
    arrived = over_owners(terms, "ka")
    weights = [wide]
    left = lax.ppermute(wide, PB, [(p, (p + 2) % groups) for p in range(groups)])
    right = lax.ppermute(wide, PB, [(p, p - 2) for p in range(2, groups)])
    far = lax.ppermute(left, PB, [(p, (p + 2) % groups) for p in (0, 1, 2, 3, 6, 7)])
    weights += [left, far, right]
    (copies,) = call(receive_kernel, [VMEM], [((groups, BANDS + 8, TILES), BF16)])(arrived)
    parts = lax.all_to_all(copies, PB, split_axis=0, concat_axis=0, tiled=True)
    terms, targets = call(
        first_kernel, [VMEM] * 6, [((2, TILES, TILES), BF16), ((8, TILES), F32)], small
    )(parts, state, *weights)
    for copied in (2, 1):
        arrived = over_owners(terms, ("core", "ka"))
        (terms,) = call(step_kernel, [VMEM] * 7, [((copied, TILES, TILES), BF16)], small)(
            arrived, targets, state, *weights
        )
    arrived = over_owners(terms, "ka")
    (copies,) = call(last_kernel, [VMEM] * 2, [((groups, BANDS, TILES), BF16)])(arrived, targets)
    parts = lax.all_to_all(copies, PB, split_axis=0, concat_axis=0, tiled=True)
    (deviation,) = call(final_kernel, [VMEM] * 2, [((ROWS, TILES), F32)])(parts, state)
    return deviation.reshape(3, BANDS, TILES)


def solution(mesh):
    fine = jax.sharding.Mesh(mesh.devices.reshape(4, 2, -1), (*PB, "ka"))
    placed = (
        P(PB, "ka", None, None, None),
        P(PB, "ka", None, None),
        P(PB, "ka", None, None),
        P(PB, "ka", None),
        P(PB, "ka", None),
        P(PB, "ka", None),
        P(None, None, "ka"),
        P(None, "ka"),
    )
    return jax.shard_map(
        shards, mesh=fine, in_specs=placed, out_specs=P(None, None, "ka"), check_vma=False
    )
```

```python
import jax
import jax.numpy as jnp
from jax import lax
from jax.experimental import pallas as pl
from jax.experimental.pallas import tpu as pltpu
from jax.sharding import PartitionSpec as P


MODES = 12
TILE_SLOTS = 2
BANDS = 32
ROWS = 3 * BANDS
TILES = 128
LANES = BANDS * MODES
CHUNKS = (24, 48, 56)
PB = ("x", "core")
WIDE = BANDS * BANDS
F32 = jnp.float32
BF16 = jnp.bfloat16


def iota(shape, axis):
    return lax.broadcasted_iota(jnp.int32, shape, axis)


def band_terms(weight, base, pairs, half_ref, term_ref, slot):
    for q in range(8):
        total = None
        for m, pair in enumerate(pairs):
            term = weight[pl.ds(q * TILES + m * 8, 8), :].astype(F32) * pair
            total = term if total is None else total + term
        half_ref[pl.ds(base + q * 8, 8), :] = total
    for j in range(4):
        term_ref[pl.ds(slot * BANDS + j * 8, 8), :] = (
            half_ref[pl.ds(base + j, 8, stride=8), :] + half_ref[pl.ds(base + j + 4, 8, stride=8), :]
        )


def band_pairs(chosen_ref, slot):
    first = iota((8, TILES), 0) < 4
    pairs = []
    for m in range(0, BANDS, 2):
        row = slot * BANDS + m
        low = jnp.broadcast_to(chosen_ref[pl.ds(row, 1), :], (8, TILES))
        high = jnp.broadcast_to(chosen_ref[pl.ds(row + 1, 1), :], (8, TILES))
        pairs.append(jnp.where(first, low, high))
    return pairs


def onehot(equal):
    return equal.astype(F32).astype(BF16)


def weight_kernel(
    coupling, occ, window, count, source, target, velocity, lifetime,
    wide_ref, out_ref, state_ref,
    weight_ref, index_ref, tiles, flat, occ_wide, occ_rows_ref, occ_pad, window_ref, count_ref, mask_ref, chosen_ref, half_ref, term_ref, sems, small_sems,
):
    small = []
    for place, (origin, into) in enumerate((
        (occ, occ_rows_ref),
        (count, count_ref),
        (window, window_ref),
        (velocity, state_ref.at[pl.ds(0, ROWS)]),
        (lifetime, state_ref.at[pl.ds(ROWS, BANDS)]),
        (source, index_ref.at[pl.ds(0, 1)]),
        (target, index_ref.at[pl.ds(1, 1)]),
    )):
        small.append(pltpu.make_async_copy(origin, into, small_sems.at[place]))
    begin = [sum(CHUNKS[:c]) for c in range(len(CHUNKS))]
    copies = []
    for c, size in enumerate(CHUNKS):
        part = pl.ds(begin[c], size)
        copies.append(pltpu.make_async_copy(coupling.at[part], tiles.at[part], sems.at[c]))
        copies[-1].start()
        if c == 0:
            for copy in small[:1]:
                copy.start()
    for copy in small[1:]:
        copy.start()
    spread = (iota((16, LANES), 1) % MODES == iota((16, LANES), 0)).astype(F32).astype(BF16)
    gather = (iota((LANES, TILES), 0) // MODES == iota((LANES, TILES), 1) // 4).astype(F32).astype(BF16)
    group = iota((1, TILES), 1) % 4
    for copy in small[:1]:
        copy.wait()
    for v in range(MODES):
        occ_pad[pl.ds(v, 1), :] = occ_rows_ref[v]
    valid = iota((16, TILES), 0) < MODES
    occ_rows = jnp.where(valid, occ_pad[...], 0.0).T.astype(BF16)
    occ_wide[...] = jnp.dot(occ_rows, spread, preferred_element_type=F32)
    for c, size in enumerate(CHUNKS):
        copies[c].wait()
        rows = []
        for t in range(begin[c], begin[c] + size):
            tile = tiles[t]
            wide = jnp.broadcast_to(occ_wide[pl.ds(t, 1), :], (BANDS, LANES)).astype(BF16)
            rows.append(tile * tile * wide)
        summed = jnp.dot(jnp.concatenate(rows, axis=0), gather, preferred_element_type=F32)
        for t in range(size):
            merged = summed[t * BANDS : t * BANDS + 8, :]
            for j in range(1, 4):
                row = t * BANDS + j * 8
                merged = jnp.where(group == j, summed[row : row + 8, :], merged)
            flat[pl.ds((begin[c] + t) * 8, 8), :] = merged
    for copy in small[1:]:
        copy.wait()
    count = count_ref[...].astype(F32).astype(BF16)
    owner = (iota((64, TILES), 1) // TILE_SLOTS == iota((64, TILES), 0)).astype(F32).astype(BF16)
    live = jnp.dot(jnp.broadcast_to(count, (8, 64)), owner, preferred_element_type=F32)
    slot = (iota((8, TILES), 1) % TILE_SLOTS).astype(F32)
    live = (slot < live).astype(F32)
    mask = window_ref[...].astype(F32) * live[0:1, :]
    mask_ref[pl.ds(0, BANDS), :] = mask
    mask_ref[pl.ds(BANDS, BANDS), :] = mask
    for q in range(8):
        turned = flat[pl.ds(q, TILES, stride=8), :].T
        rows = mask_ref[pl.ds(q, 8, stride=8), :]
        for m in range(16):
            weight_ref[pl.ds(q * TILES + m * 8, 8), :] = turned[m * 8 : m * 8 + 8, :] * rows
    source_row = jnp.broadcast_to(index_ref[0:1, :], (16, TILES))
    wide_ref[pl.ds(0, WIDE), :] = weight_ref[...].astype(BF16)
    wide_ref[pl.ds(WIDE, 16), :] = source_row.astype(F32).astype(BF16)
    lifetime_now = state_ref[pl.ds(ROWS, BANDS), :]
    deviation = jnp.concatenate(
        [lifetime_now * state_ref[pl.ds(i * BANDS, BANDS), :] for i in range(3)], axis=0
    )
    picks = onehot(iota((TILES, TILES), 0) == index_ref[0:1, :])
    chosen_ref[...] = jnp.dot(deviation.astype(BF16), picks, preferred_element_type=F32)
    for i in range(3):
        band_terms(weight_ref, i * 64, band_pairs(chosen_ref, i), half_ref, term_ref, i)
    target = index_ref[1:2, :].astype(F32)
    term_ref[pl.ds(ROWS, BANDS), :] = jnp.where(iota((BANDS, TILES), 0) == 0, target, 0.0)
    out_ref[...] = term_ref[...].T.astype(BF16)


def receive_kernel(terms_ref, out_ref):
    terms = terms_ref[...].astype(F32)
    target = terms[:, ROWS : ROWS + 1].astype(jnp.int32)
    turned = terms.T
    places = onehot(iota((TILES, TILES), 1) == target)
    total = jnp.dot(turned[:ROWS, :].astype(BF16), places, preferred_element_type=F32)
    targets = turned[ROWS : ROWS + 8, :]
    messages = [
        jnp.concatenate([total[i * BANDS : (i + 1) * BANDS, :], targets], axis=0).astype(BF16)
        for i in range(3)
    ]
    for p in range(out_ref.shape[0]):
        out_ref[p] = messages[p // 2 % 3]


def direction_terms(deviation, weights, chosen_ref, half_ref, term_ref, out_ref):
    picks = []
    for weight in weights:
        source_row = weight[pl.ds(WIDE, 16), :].astype(F32)[0:1, :].astype(jnp.int32)
        picks.append(onehot(iota((TILES, TILES), 0) == source_row))
    chosen = jnp.dot(deviation.astype(BF16), jnp.concatenate(picks, axis=1), preferred_element_type=F32)
    for g, weight in enumerate(weights):
        chosen_ref[pl.ds(g * BANDS, BANDS), :] = chosen[:, g * TILES : (g + 1) * TILES]
    for g, weight in enumerate(weights):
        band_terms(weight, g * 64, band_pairs(chosen_ref, g), half_ref, term_ref, g)
    message = term_ref[...].T.astype(BF16)
    for core in range(out_ref.shape[0]):
        out_ref[core] = message


def own_direction():
    return lax.axis_index("x") % 3


def next_direction(state_ref, scattering):
    rows = pl.ds(pl.multiple_of(own_direction() * BANDS, BANDS), BANDS)
    return state_ref[pl.ds(ROWS, BANDS), :] * (state_ref[rows, :] + scattering)


def first_kernel(parts_ref, state_ref, w0, w1, w2, w3, out_ref, target_ref, chosen_ref, half_ref, term_ref):
    total = parts_ref[0, pl.ds(0, BANDS), :].astype(F32)
    for p in range(1, parts_ref.shape[0]):
        total = total + parts_ref[p, pl.ds(0, BANDS), :].astype(F32)
    for g in range(4):
        for core in range(2):
            peer = 2 * lax.rem(lax.axis_index("x") + 4 - g, 4) + core
            row = parts_ref[peer, pl.ds(BANDS, 8), :].astype(F32)[0:1, :]
            target_ref[pl.ds(2 * g + core, 1), :] = row
    deviation = next_direction(state_ref, total)
    direction_terms(deviation, (w0, w1, w2, w3), chosen_ref, half_ref, term_ref, out_ref)


def direction_sum(terms_ref, target_ref, cores):
    turned = terms_ref[...].astype(F32).T.astype(BF16)
    left, right = [], []
    for g in range(4):
        left.append(turned[g * BANDS : (g + 1) * BANDS, :])
        for core in cores:
            target = target_ref[pl.ds(2 * g + core, 1), :].astype(jnp.int32)
            right.append(onehot(iota((TILES, TILES), 0) == target))
    return lax.dot_general(
        jnp.concatenate(left, axis=1), jnp.concatenate(right, axis=1), (((1,), (1,)), ((), ())),
        preferred_element_type=F32,
    )


def step_kernel(terms_ref, target_ref, state_ref, w0, w1, w2, w3, out_ref, chosen_ref, half_ref, term_ref):
    deviation = next_direction(state_ref, direction_sum(terms_ref, target_ref, (0, 1)))
    direction_terms(deviation, (w0, w1, w2, w3), chosen_ref, half_ref, term_ref, out_ref)


def last_kernel(terms_ref, target_ref, out_ref):
    total = direction_sum(terms_ref, target_ref, (lax.axis_index("core"),)).astype(BF16)
    for p in range(out_ref.shape[0]):
        out_ref[p] = total


def final_kernel(parts_ref, state_ref, out_ref):
    for i in range(3):
        total = parts_ref[2 * i].astype(F32) + parts_ref[2 * i + 1].astype(F32)
        rows = pl.ds(i * BANDS, BANDS)
        out_ref[rows, :] = state_ref[pl.ds(ROWS, BANDS), :] * (state_ref[rows, :] + total)


VMEM = pl.BlockSpec(memory_space=pltpu.VMEM)


def call(body, ins, outs, scratch=(), limit=4 << 20, flops=1000000):
    return pl.pallas_call(
        body,
        in_specs=ins,
        out_specs=[VMEM] * len(outs),
        out_shape=[jax.ShapeDtypeStruct(s, d) for s, d in outs],
        scratch_shapes=list(scratch),
        compiler_params=pltpu.CompilerParams(vmem_limit_bytes=limit),
        cost_estimate=pl.CostEstimate(flops=flops, bytes_accessed=1 << 20, transcendentals=0),
    )


def over_owners(terms, axes):
    return lax.all_to_all(
        terms.reshape(-1, TILE_SLOTS, TILES), axes, split_axis=0, concat_axis=0, tiled=True
    ).reshape(-1, TILES)


def shards(coupling, phonon_occ, band_window, pair_count, k_target, kq_source, velocity, lifetime):
    groups = lax.axis_size("x") * lax.axis_size("core")
    small = [
        pltpu.VMEM((TILES, TILES), F32), pltpu.VMEM((4 * 64, TILES), F32), pltpu.VMEM((TILES, TILES), F32)
    ]
    wide, terms, state = call(
        weight_kernel, [pl.BlockSpec(memory_space=pltpu.HBM)] * 8,
        [((WIDE + 16, TILES), BF16), ((TILES, TILES), BF16), ((TILES, TILES), F32)],
        [
            pltpu.VMEM((WIDE, TILES), F32),
            pltpu.VMEM((8, TILES), jnp.int32),
            pltpu.VMEM((TILES, BANDS, LANES), BF16),
            pltpu.VMEM((TILES * 8, TILES), F32),
            pltpu.VMEM((TILES, LANES), F32),
            pltpu.VMEM((MODES, 1, TILES), F32),
            pltpu.VMEM((16, TILES), F32),
            pltpu.VMEM((BANDS, TILES), jnp.int32),
            pltpu.VMEM((1, 64), jnp.int32),
            pltpu.VMEM((2 * BANDS, TILES), F32),
            pltpu.VMEM((ROWS, TILES), F32), *small[1:],
            pltpu.SemaphoreType.DMA((len(CHUNKS),)),
            pltpu.SemaphoreType.DMA((7,)),
        ],
        limit=16 << 20,
    )(*(pltpu.with_memory_space_constraint(x, pltpu.HBM) for x in (
        coupling[0, 0], phonon_occ.transpose(0, 3, 1, 2).reshape(MODES, 1, TILES), band_window[0, 0].T, pair_count[0],
        kq_source.reshape(1, TILES), k_target.reshape(1, TILES), velocity.reshape(ROWS, TILES), lifetime,
    )))
    arrived = over_owners(terms, "ka")
    weights = [wide]
    left = lax.ppermute(wide, PB, [(p, (p + 2) % groups) for p in range(groups)])
    right = lax.ppermute(wide, PB, [(p, p - 2) for p in range(2, groups)])
    far = lax.ppermute(left, PB, [(p, (p + 2) % groups) for p in (0, 1, 2, 3, 6, 7)])
    weights += [left, far, right]
    (copies,) = call(receive_kernel, [VMEM], [((groups, BANDS + 8, TILES), BF16)])(arrived)
    parts = lax.all_to_all(copies, PB, split_axis=0, concat_axis=0, tiled=True)
    terms, targets = call(
        first_kernel, [VMEM] * 6, [((2, TILES, TILES), BF16), ((8, TILES), F32)], small
    )(parts, state, *weights)
    for copied in (2, 1):
        arrived = over_owners(terms, ("core", "ka"))
        (terms,) = call(step_kernel, [VMEM] * 7, [((copied, TILES, TILES), BF16)], small)(
            arrived, targets, state, *weights
        )
    arrived = over_owners(terms, "ka")
    (copies,) = call(last_kernel, [VMEM] * 2, [((groups, BANDS, TILES), BF16)])(arrived, targets)
    parts = lax.all_to_all(copies, PB, split_axis=0, concat_axis=0, tiled=True)
    (deviation,) = call(final_kernel, [VMEM] * 2, [((ROWS, TILES), F32)])(parts, state)
    return deviation.reshape(3, BANDS, TILES)


def solution(mesh):
    fine = jax.sharding.Mesh(mesh.devices.reshape(4, 2, -1), (*PB, "ka"))
    placed = (
        P(PB, "ka", None, None, None),
        P(PB, "ka", None, None),
        P(PB, "ka", None, None),
        P(PB, "ka", None),
        P(PB, "ka", None),
        P(PB, "ka", None),
        P(None, None, "ka"),
        P(None, "ka"),
    )
    return jax.shard_map(
        shards, mesh=fine, in_specs=placed, out_specs=P(None, None, "ka"), check_vma=False
    )
```

```python
import jax
import jax.numpy as jnp
from jax import lax
from jax.experimental import pallas as pl
from jax.experimental.pallas import tpu as pltpu
from jax.sharding import PartitionSpec as P


MODES = 12
TILE_SLOTS = 2
BANDS = 32
ROWS = 3 * BANDS
TILES = 128
LANES = BANDS * MODES
CHUNKS = (24, 48, 56)
PB = ("x", "core")
WIDE = BANDS * BANDS
F32 = jnp.float32
BF16 = jnp.bfloat16


def iota(shape, axis):
    return lax.broadcasted_iota(jnp.int32, shape, axis)


def band_terms(weight, base, pairs, half_ref, term_ref, slot):
    for q in range(8):
        total = None
        for m, pair in enumerate(pairs):
            term = weight[pl.ds(q * TILES + m * 8, 8), :].astype(F32) * pair
            total = term if total is None else total + term
        half_ref[pl.ds(base + q * 8, 8), :] = total
    for j in range(4):
        term_ref[pl.ds(slot * BANDS + j * 8, 8), :] = (
            half_ref[pl.ds(base + j, 8, stride=8), :] + half_ref[pl.ds(base + j + 4, 8, stride=8), :]
        )


def band_pairs(chosen_ref, slot):
    first = iota((8, TILES), 0) < 4
    pairs = []
    for m in range(0, BANDS, 2):
        row = slot * BANDS + m
        low = jnp.broadcast_to(chosen_ref[pl.ds(row, 1), :], (8, TILES))
        high = jnp.broadcast_to(chosen_ref[pl.ds(row + 1, 1), :], (8, TILES))
        pairs.append(jnp.where(first, low, high))
    return pairs


def onehot(equal):
    return equal.astype(F32).astype(BF16)


def weight_kernel(
    coupling, occ, window, count, source, target, velocity, lifetime,
    wide_ref, out_ref, state_ref,
    weight_ref, index_ref, tiles, flat, occ_wide, occ_rows_ref, occ_pad, window_ref, count_ref, mask_ref, chosen_ref, half_ref, term_ref, sems, small_sems,
):
    small = []
    for place, (origin, into) in enumerate((
        (occ, occ_rows_ref),
        (count, count_ref),
        (window, window_ref),
        (velocity, state_ref.at[pl.ds(0, ROWS)]),
        (lifetime, state_ref.at[pl.ds(ROWS, BANDS)]),
        (source, index_ref.at[pl.ds(0, 1)]),
        (target, index_ref.at[pl.ds(1, 1)]),
    )):
        small.append(pltpu.make_async_copy(origin, into, small_sems.at[place]))
    begin = [sum(CHUNKS[:c]) for c in range(len(CHUNKS))]
    copies = []
    for c, size in enumerate(CHUNKS):
        part = pl.ds(begin[c], size)
        copies.append(pltpu.make_async_copy(coupling.at[part], tiles.at[part], sems.at[c]))
        copies[-1].start()
        if c == 0:
            for copy in small[:1]:
                copy.start()
    for copy in small[1:]:
        copy.start()
    spread = (iota((16, LANES), 1) % MODES == iota((16, LANES), 0)).astype(F32).astype(BF16)
    gather = (iota((LANES, TILES), 0) // MODES == iota((LANES, TILES), 1) // 4).astype(F32).astype(BF16)
    group = iota((1, TILES), 1) % 4
    for copy in small[:1]:
        copy.wait()
    for v in range(MODES):
        occ_pad[pl.ds(v, 1), :] = occ_rows_ref[v]
    valid = iota((16, TILES), 0) < MODES
    occ_rows = jnp.where(valid, occ_pad[...], 0.0).T.astype(BF16)
    occ_wide[...] = jnp.dot(occ_rows, spread, preferred_element_type=F32)
    for c, size in enumerate(CHUNKS):
        copies[c].wait()
        rows = []
        for t in range(begin[c], begin[c] + size):
            tile = tiles[t]
            wide = jnp.broadcast_to(occ_wide[pl.ds(t, 1), :], (BANDS, LANES)).astype(BF16)
            rows.append(tile * tile * wide)
        summed = jnp.dot(jnp.concatenate(rows, axis=0), gather, preferred_element_type=F32)
        for t in range(size):
            merged = summed[t * BANDS : t * BANDS + 8, :]
            for j in range(1, 4):
                row = t * BANDS + j * 8
                merged = jnp.where(group == j, summed[row : row + 8, :], merged)
            flat[pl.ds((begin[c] + t) * 8, 8), :] = merged
    for copy in small[1:]:
        copy.wait()
    count = count_ref[...].astype(F32).astype(BF16)
    owner = (iota((64, TILES), 1) // TILE_SLOTS == iota((64, TILES), 0)).astype(F32).astype(BF16)
    live = jnp.dot(jnp.broadcast_to(count, (8, 64)), owner, preferred_element_type=F32)
    slot = (iota((8, TILES), 1) % TILE_SLOTS).astype(F32)
    live = (slot < live).astype(F32)
    mask = window_ref[...].astype(F32) * live[0:1, :]
    mask_ref[pl.ds(0, BANDS), :] = mask
    mask_ref[pl.ds(BANDS, BANDS), :] = mask
    for q in range(8):
        turned = flat[pl.ds(q, TILES, stride=8), :].T
        rows = mask_ref[pl.ds(q, 8, stride=8), :]
        for m in range(16):
            weight_ref[pl.ds(q * TILES + m * 8, 8), :] = turned[m * 8 : m * 8 + 8, :] * rows
    source_row = jnp.broadcast_to(index_ref[0:1, :], (16, TILES))
    wide_ref[pl.ds(0, WIDE), :] = weight_ref[...].astype(BF16)
    wide_ref[pl.ds(WIDE, 16), :] = source_row.astype(F32).astype(BF16)
    lifetime_now = state_ref[pl.ds(ROWS, BANDS), :]
    deviation = jnp.concatenate(
        [lifetime_now * state_ref[pl.ds(i * BANDS, BANDS), :] for i in range(3)], axis=0
    )
    picks = onehot(iota((TILES, TILES), 0) == index_ref[0:1, :])
    chosen_ref[...] = jnp.dot(deviation.astype(BF16), picks, preferred_element_type=F32)
    for i in range(3):
        band_terms(weight_ref, i * 64, band_pairs(chosen_ref, i), half_ref, term_ref, i)
    target = index_ref[1:2, :].astype(F32)
    term_ref[pl.ds(ROWS, BANDS), :] = jnp.where(iota((BANDS, TILES), 0) == 0, target, 0.0)
    out_ref[...] = term_ref[...].T.astype(BF16)


def receive_kernel(terms_ref, out_ref):
    terms = terms_ref[...].astype(F32)
    target = terms[:, ROWS : ROWS + 1].astype(jnp.int32)
    turned = terms.T
    places = onehot(iota((TILES, TILES), 1) == target)
    total = jnp.dot(turned[:ROWS, :].astype(BF16), places, preferred_element_type=F32)
    targets = turned[ROWS : ROWS + 8, :]
    messages = [
        jnp.concatenate([total[i * BANDS : (i + 1) * BANDS, :], targets], axis=0).astype(BF16)
        for i in range(3)
    ]
    for p in range(out_ref.shape[0]):
        out_ref[p] = messages[p // 2 % 3]


def direction_terms(deviation, picks, weights, chosen_ref, half_ref, term_ref, out_ref):
    chosen = jnp.dot(deviation.astype(BF16), picks, preferred_element_type=F32)
    for g, weight in enumerate(weights):
        chosen_ref[pl.ds(g * BANDS, BANDS), :] = chosen[:, g * TILES : (g + 1) * TILES]
    for g, weight in enumerate(weights):
        band_terms(weight, g * 64, band_pairs(chosen_ref, g), half_ref, term_ref, g)
    message = term_ref[...].T.astype(BF16)
    for core in range(out_ref.shape[0]):
        out_ref[core] = message


def own_direction():
    return lax.axis_index("x") % 3


def next_direction(state_ref, scattering):
    rows = pl.ds(pl.multiple_of(own_direction() * BANDS, BANDS), BANDS)
    return state_ref[pl.ds(ROWS, BANDS), :] * (state_ref[rows, :] + scattering)


def first_kernel(parts_ref, state_ref, w0, w1, w2, w3, out_ref, place_ref, pick_ref, chosen_ref, half_ref, term_ref):
    total = parts_ref[0, pl.ds(0, BANDS), :].astype(F32)
    for p in range(1, parts_ref.shape[0]):
        total = total + parts_ref[p, pl.ds(0, BANDS), :].astype(F32)
    for g in range(4):
        for core in range(2):
            peer = 2 * lax.rem(lax.axis_index("x") + 4 - g, 4) + core
            target = parts_ref[peer, pl.ds(BANDS, 8), :].astype(F32)[0:1, :].astype(jnp.int32)
            columns = pl.ds((2 * g + core) * TILES, TILES)
            place_ref[:, columns] = onehot(iota((TILES, TILES), 0) == target)
    for g, weight in enumerate((w0, w1, w2, w3)):
        source_row = weight[pl.ds(WIDE, 16), :].astype(F32)[0:1, :].astype(jnp.int32)
        pick_ref[:, pl.ds(g * TILES, TILES)] = onehot(iota((TILES, TILES), 0) == source_row)
    deviation = next_direction(state_ref, total)
    direction_terms(deviation, pick_ref[...], (w0, w1, w2, w3), chosen_ref, half_ref, term_ref, out_ref)


def direction_sum(terms_ref, place_ref, cores):
    turned = terms_ref[...].astype(F32).T.astype(BF16)
    left, right = [], []
    for g in range(4):
        left.append(turned[g * BANDS : (g + 1) * BANDS, :])
        for core in cores:
            start = (2 * g + core) * TILES
            right.append(place_ref[:, pl.ds(pl.multiple_of(start, TILES), TILES)])
    return lax.dot_general(
        jnp.concatenate(left, axis=1), jnp.concatenate(right, axis=1), (((1,), (1,)), ((), ())),
        preferred_element_type=F32,
    )


def step_kernel(terms_ref, place_ref, pick_ref, state_ref, w0, w1, w2, w3, out_ref, chosen_ref, half_ref, term_ref):
    deviation = next_direction(state_ref, direction_sum(terms_ref, place_ref, (0, 1)))
    direction_terms(deviation, pick_ref[...], (w0, w1, w2, w3), chosen_ref, half_ref, term_ref, out_ref)


def last_kernel(terms_ref, place_ref, out_ref):
    total = direction_sum(terms_ref, place_ref, (lax.axis_index("core"),)).astype(BF16)
    for p in range(out_ref.shape[0]):
        out_ref[p] = total


def final_kernel(parts_ref, state_ref, out_ref):
    for i in range(3):
        total = parts_ref[2 * i].astype(F32) + parts_ref[2 * i + 1].astype(F32)
        rows = pl.ds(i * BANDS, BANDS)
        out_ref[rows, :] = state_ref[pl.ds(ROWS, BANDS), :] * (state_ref[rows, :] + total)


VMEM = pl.BlockSpec(memory_space=pltpu.VMEM)


def call(body, ins, outs, scratch=(), limit=4 << 20, flops=1000000):
    return pl.pallas_call(
        body,
        in_specs=ins,
        out_specs=[VMEM] * len(outs),
        out_shape=[jax.ShapeDtypeStruct(s, d) for s, d in outs],
        scratch_shapes=list(scratch),
        compiler_params=pltpu.CompilerParams(vmem_limit_bytes=limit),
        cost_estimate=pl.CostEstimate(flops=flops, bytes_accessed=1 << 20, transcendentals=0),
    )


def over_owners(terms, axes):
    return lax.all_to_all(
        terms.reshape(-1, TILE_SLOTS, TILES), axes, split_axis=0, concat_axis=0, tiled=True
    ).reshape(-1, TILES)


def shards(coupling, phonon_occ, band_window, pair_count, k_target, kq_source, velocity, lifetime):
    groups = lax.axis_size("x") * lax.axis_size("core")
    small = [
        pltpu.VMEM((TILES, TILES), F32), pltpu.VMEM((4 * 64, TILES), F32), pltpu.VMEM((TILES, TILES), F32)
    ]
    wide, terms, state = call(
        weight_kernel, [pl.BlockSpec(memory_space=pltpu.HBM)] * 8,
        [((WIDE + 16, TILES), BF16), ((TILES, TILES), BF16), ((TILES, TILES), F32)],
        [
            pltpu.VMEM((WIDE, TILES), F32),
            pltpu.VMEM((8, TILES), jnp.int32),
            pltpu.VMEM((TILES, BANDS, LANES), BF16),
            pltpu.VMEM((TILES * 8, TILES), F32),
            pltpu.VMEM((TILES, LANES), F32),
            pltpu.VMEM((MODES, 1, TILES), F32),
            pltpu.VMEM((16, TILES), F32),
            pltpu.VMEM((BANDS, TILES), jnp.int32),
            pltpu.VMEM((1, 64), jnp.int32),
            pltpu.VMEM((2 * BANDS, TILES), F32),
            pltpu.VMEM((ROWS, TILES), F32), *small[1:],
            pltpu.SemaphoreType.DMA((len(CHUNKS),)),
            pltpu.SemaphoreType.DMA((7,)),
        ],
        limit=16 << 20,
    )(*(pltpu.with_memory_space_constraint(x, pltpu.HBM) for x in (
        coupling[0, 0], phonon_occ.transpose(0, 3, 1, 2).reshape(MODES, 1, TILES), band_window[0, 0].T, pair_count[0],
        kq_source.reshape(1, TILES), k_target.reshape(1, TILES), velocity.reshape(ROWS, TILES), lifetime,
    )))
    arrived = over_owners(terms, "ka")
    weights = [wide]
    left = lax.ppermute(wide, PB, [(p, (p + 2) % groups) for p in range(groups)])
    right = lax.ppermute(wide, PB, [(p, p - 2) for p in range(2, groups)])
    far = lax.ppermute(left, PB, [(p, (p + 2) % groups) for p in (0, 1, 2, 3, 6, 7)])
    weights += [left, far, right]
    (copies,) = call(receive_kernel, [VMEM], [((groups, BANDS + 8, TILES), BF16)])(arrived)
    parts = lax.all_to_all(copies, PB, split_axis=0, concat_axis=0, tiled=True)
    terms, places, picks = call(
        first_kernel, [VMEM] * 6, [((2, TILES, TILES), BF16), ((TILES, 8 * TILES), BF16), ((TILES, 4 * TILES), BF16)], small
    )(parts, state, *weights)
    for copied in (2, 1):
        arrived = over_owners(terms, ("core", "ka"))
        (terms,) = call(step_kernel, [VMEM] * 8, [((copied, TILES, TILES), BF16)], small)(
            arrived, places, picks, state, *weights
        )
    arrived = over_owners(terms, "ka")
    (copies,) = call(last_kernel, [VMEM] * 2, [((groups, BANDS, TILES), BF16)])(arrived, places)
    parts = lax.all_to_all(copies, PB, split_axis=0, concat_axis=0, tiled=True)
    (deviation,) = call(final_kernel, [VMEM] * 2, [((ROWS, TILES), F32)])(parts, state)
    return deviation.reshape(3, BANDS, TILES)


def solution(mesh):
    fine = jax.sharding.Mesh(mesh.devices.reshape(4, 2, -1), (*PB, "ka"))
    placed = (
        P(PB, "ka", None, None, None),
        P(PB, "ka", None, None),
        P(PB, "ka", None, None),
        P(PB, "ka", None),
        P(PB, "ka", None),
        P(PB, "ka", None),
        P(None, None, "ka"),
        P(None, "ka"),
    )
    return jax.shard_map(
        shards, mesh=fine, in_specs=placed, out_specs=P(None, None, "ka"), check_vma=False
    )
```
